32 devices in a mesh: gx: 8 (over z, x), gy: 4 (over y, core).
Axes of the slice: x: 2, y: 2, z: 4, core: 2. Of those that a mesh axis runs over, the one named last changes fastest.
Arguments:
- species: float32 [53, 32, 32, 128], P(None, 'gx', 'gy'), may hold values from -6 to 6
- diffusion: float32 [53], replicated, may hold values from 0.02 to 0.15
- class_rate: float32 [4], replicated, may hold values from 0.2 to 1
- mixing: float32 [53, 53], replicated, may hold values from -0.3 to 0.3
- inverses: float32 [4, 53, 53], replicated, may hold values from -0.01 to 0.12
- newton_counts: int32 [4], replicated, may hold values from 1 to 8, as said below
- cell_class: int32 [32, 32, 128], P('gx', 'gy'), may hold values from 0 to 3
Outputs:
- updated: float32 [53, 32, 32, 128], P(None, 'gx', 'gy')
The draws below stay inside these ranges and needn't reach their ends.
Inputs may be any that keep to these rules, and one draw needn't show every extreme that they name: `newton_counts`: nondecreasing in the class; the last class takes 8.
All inputs are finite; a program needn't handle non-finite values.
Results may differ from the reference program's by a relative error of at most 0.0003.
Values sent between devices are 32-bit elements; how exact they have to be, the bound alone decides.
No kernel may reach another device: no remote copies, remote signals or barrier semaphores. Data moves between devices by JAX's collectives and lax.ppermute only.
A program may use at most 64 MiB of HBM per device.

```python
import math
import jax
import jax.numpy as jnp
from jax import lax

SPEC = 53
NCLASS = 4
NMAX = 8
NZ = 128
NX = 32
NY = 32


def draw_inverses(key, part):
    first, second = jax.random.split(jax.random.fold_in(key, 5))
    diag = jnp.exp(jax.random.uniform(first, (NCLASS, SPEC), jnp.float32, math.log(0.06), math.log(0.12)))
    spread = jax.random.normal(second, (NCLASS, SPEC, SPEC), jnp.float32)
    spread = jnp.clip(spread * (0.0225 / math.sqrt(SPEC)), -0.01, 0.01)
    identity = jnp.eye(SPEC, dtype=jnp.float32)[None]
    return spread * (1.0 - identity) + diag[:, :, None] * identity


def draw_newton_counts(key, part):
    base = jax.random.randint(jax.random.fold_in(key, 11), (NCLASS,), 1, NMAX + 1)
    base = jnp.sort(base)
    return base.at[NCLASS - 1].set(NMAX).astype(jnp.int32)


def draw_cell_class(key, part):
    front_key, heavy_key, pick_key, light_key = jax.random.split(jax.random.fold_in(key, 23), 4)
    front = jax.random.randint(front_key, (), 0, NX)
    positions = jnp.arange(NX, dtype=jnp.int32)[:, None, None]
    near = jnp.abs(positions - front) < max(NX // 16, 1)
    shape = (NX, NY, NZ)
    heavy = jax.random.randint(heavy_key, shape, 1, NCLASS)
    picked = jax.random.randint(pick_key, shape, 0, 8)
    light = jnp.where(picked == 0, jax.random.randint(light_key, shape, 0, NCLASS), 0)
    return jnp.where(near, heavy, light).astype(jnp.int32)


def level_of(stream_key, shape, shards, least, largest):
    gain = 1.0
    for dim, shards_of in shards:
        draws = jax.random.uniform(jax.random.fold_in(jax.random.fold_in(stream_key, 6), dim), (shards_of,), jnp.float32, least / len(shards), largest / len(shards))
        gain = gain * jnp.repeat(jnp.exp(draws), shape[dim] // shards_of).reshape((-1,) + (1,) * (len(shape) - 1 - dim))
    return gain


def normal_values(own_key, extent, scale, bound, cuts=(), held_as=jnp.bfloat16):
    level = level_of(own_key, extent, cuts, -0.22, 0.18) if cuts else 1.0
    values = jax.random.normal(own_key, extent, jnp.float32) * scale * level
    return jnp.minimum(jnp.maximum(values, -bound), bound).astype(held_as)


def setup_inputs(seed: int = 0) -> dict:
    arg_keys = jax.random.split(jax.random.key(seed), 8)
    species = normal_values(arg_keys[0], (SPEC, NX, NY, NZ), 1.0, 6.0, ((1, 8), (2, 4)), jnp.float32)
    diffusion = jnp.clip(jnp.exp(jax.random.uniform(arg_keys[1], (SPEC,), jnp.float32, math.log(0.02), math.log(0.15))), 0.02, 0.15)
    class_rate = jnp.clip(jnp.exp(jax.random.uniform(arg_keys[2], (NCLASS,), jnp.float32, math.log(0.2), math.log(1.0))), 0.2, 1.0)
    mixing = normal_values(arg_keys[3], (SPEC, SPEC), (0.3 * SPEC ** -0.5), 0.3, (), jnp.float32)
    inverses = draw_inverses(jax.random.fold_in(arg_keys[7], 71), 0)
    newton_counts = draw_newton_counts(jax.random.fold_in(arg_keys[7], 71), 0)
    cell_class = draw_cell_class(jax.random.fold_in(arg_keys[7], 71), 0)
    return {"species": species, "diffusion": diffusion, "class_rate": class_rate, "mixing": mixing, "inverses": inverses, "newton_counts": newton_counts, "cell_class": cell_class}


def laplace(grid_field):
    padded = jnp.pad(grid_field, 1)
    total = padded[2:, 1:-1, 1:-1] + padded[:-2, 1:-1, 1:-1]
    total = total + padded[1:-1, 2:, 1:-1] + padded[1:-1, :-2, 1:-1]
    total = total + padded[1:-1, 1:-1, 2:] + padded[1:-1, 1:-1, :-2]
    return total - 6.0 * grid_field


def newton_cells(target, classes, class_rate, mixing, inverses, newton_counts):
    class_mask = (classes[None, :] == jnp.arange(NCLASS, dtype=jnp.int32)[:, None])
    weights = class_mask.astype(jnp.float32)
    cell_rate = jnp.sum(class_rate[:, None] * weights, axis=0)
    cell_count = jnp.sum(jnp.where(class_mask, newton_counts[:, None], 0), axis=0)

    def newton_step(k, state):
        source = jnp.dot(mixing, jnp.tanh(state), precision=lax.Precision.HIGHEST) - state
        residual = state - target - cell_rate * source
        correction = jnp.zeros_like(state)
        for which in range(NCLASS):
            correction = correction + weights[which] * jnp.dot(inverses[which], residual, precision=lax.Precision.HIGHEST)
        return jnp.where(k < cell_count, state - correction, state)

    return lax.fori_loop(0, NMAX, newton_step, target)


def reference(species, diffusion, class_rate, mixing, inverses, newton_counts, cell_class):
    forcing = lax.map(laplace, species) * diffusion[:, None, None, None]
    target = species + forcing
    moved = jnp.moveaxis(target, 1, 0)

    def solve_slice(pair):
        slab, slab_class = pair
        solved = newton_cells(slab.reshape(SPEC, -1), slab_class.reshape(-1), class_rate, mixing, inverses, newton_counts)
        return solved.reshape(slab.shape)

    section_value = jnp.moveaxis(lax.map(solve_slice, (moved, cell_class)), 0, 1)
    second = lax.map(laplace, section_value) * diffusion[:, None, None, None]
    return section_value + 0.5 * (second - forcing)
```

```python
import functools

import jax
import jax.numpy as jnp
from jax import lax
from jax.experimental import pallas as pl
from jax.experimental.pallas import tpu as pltpu
from jax.sharding import PartitionSpec as P

F32 = jnp.float32
BF16 = jnp.bfloat16


def up(value, step):
    return -(-value // step) * step


def swap(block, axis, first):
    count = lax.axis_size(axis)
    pairs = []
    for i in range(first, count - 1, 2):
        pairs += [(i, i + 1), (i + 1, i)]
    return lax.ppermute(block, axis, pairs)


def split(value):
    high = value.astype(BF16)
    low = (value - high.astype(F32)).astype(BF16)
    return jnp.concatenate([high, low, high], axis=0)


def packed(weights):
    high = lax.reduce_precision(weights, 8, 7)
    return jnp.concatenate([high, high, weights - high], axis=-1).astype(BF16)


def widen(value, rows):
    short = rows - value.shape[0]
    if short == 0:
        return value
    return jnp.concatenate([value, jnp.zeros((short, value.shape[1]), value.dtype)], axis=0)


def newton(tiles, y_ref, t_ref, cls_ref, rate, count, w1_ref, w2_ref, sp, deep, nclass):
    nz = y_ref.shape[-1]

    def lanes(ref, rows):
        return jnp.concatenate([ref[r] for r in rows], axis=1)

    for low in range(nclass):
        live = nclass - low

        def body(_, carry, low=low, live=live):
            mixed = []
            for rows in tiles:
                y = lanes(y_ref, rows)
                t = widen(jnp.tanh(y), deep)
                m = jnp.dot(w1_ref[...], split(t), preferred_element_type=F32)
                mixed.append(m[:sp])
            for rows, m in zip(tiles, mixed):
                y = lanes(y_ref, rows)
                target = lanes(t_ref, rows)
                kind = jnp.broadcast_to(lanes(cls_ref, rows), (8, nz * len(rows)))
                inv = jnp.full(kind.shape, 1.0 / rate[0], F32)
                for c in range(1, nclass):
                    inv = jnp.where(kind == c, 1.0 / rate[c], inv)
                inv = jnp.concatenate([inv] * (sp // 8), axis=0)
                g = (inv + 1.0) * y - inv * target - m
                w2 = w2_ref[: up(live * sp, 16), :]
                out = jnp.dot(w2, split(widen(g, deep)), preferred_element_type=F32)
                kind = jnp.concatenate([kind] * (sp // 8), axis=0)
                step = out[(live - 1) * sp : live * sp] if low == 0 else jnp.zeros_like(y)
                for j in range(live - 1 if low == 0 else live):
                    c = nclass - 1 - j
                    step = jnp.where(kind == c, out[j * sp : (j + 1) * sp], step)
                y = y - step
                for n, r in enumerate(rows):
                    y_ref[r] = y[:, n * nz : (n + 1) * nz]
            return carry

        begin = 0 if low == 0 else count[low - 1]
        lax.fori_loop(begin, count[low], body, 0)


def shifted(v):
    lane = lax.broadcasted_iota(jnp.int32, v.shape, 1)
    nz = v.shape[1]
    left = jnp.where(lane == 0, 0.0, pltpu.roll(v, 1, 1))
    right = jnp.where(lane == nz - 1, 0.0, pltpu.roll(v, nz - 1, 1))
    return left + right


def fill(pad_ref, block_ref, even, xa_ref, xb_ref, ya_ref, yb_ref, even_y, nx, ny, ns, native):
    sp, nz = pad_ref.shape[2:]
    if sp != ns:
        for x in range(nx + 2):
            for y in range(ny + 2):
                pad_ref[x, y, sp - 8 : sp, :] = jnp.zeros((8, nz), F32)
    for x in range(nx):
        for y in range(ny):
            if native:
                pad_ref[x + 1, y + 1, :ns, :] = block_ref[pl.ds(x * ny + y, ns, stride=nx * ny), :]
            else:
                pad_ref[x + 1, y + 1] = block_ref[x * ny + y]
    near = jnp.where(even == 1, nx + 1, 0)
    far = jnp.where(even == 1, 0, nx + 1)
    for y in range(ny):
        pad_ref[near, y + 1, :ns, :] = xa_ref[pl.ds(y, ns, stride=ny), :]
        pad_ref[far, y + 1, :ns, :] = xb_ref[pl.ds(y, ns, stride=ny), :]
    near = jnp.where(even_y == 1, ny + 1, 0)
    far = jnp.where(even_y == 1, 0, ny + 1)
    for x in range(nx):
        pad_ref[x + 1, near, :ns, :] = ya_ref[pl.ds(x, ns, stride=nx), :]
        pad_ref[x + 1, far, :ns, :] = yb_ref[pl.ds(x, ns, stride=nx), :]


def lap(pad_ref, x, y):
    v = pad_ref[x + 1, y + 1]
    total = pad_ref[x + 2, y + 1] + pad_ref[x, y + 1]
    total = total + pad_ref[x + 1, y + 2] + pad_ref[x + 1, y]
    return v, total + shifted(v) - 6.0 * v


def first_kernel(nx, ny, ns, nclass, flags, rate, count, sp_ref, xa, xb, ya, yb, dif, cls_ref, w1_ref, w2_ref,
                 sec_ref, for_ref, fx0, fx1, fy0, fy1, pad_ref, t_ref):
    sp, nz = pad_ref.shape[2:]
    deep = w1_ref.shape[0]
    fill(pad_ref, sp_ref, flags[0], xa, xb, ya, yb, flags[1], nx, ny, ns, True)
    scale = jnp.broadcast_to(dif[...], (sp, nz))
    for x in range(nx):
        for y in range(ny):
            v, second = lap(pad_ref, x, y)
            force = scale * second
            r = x * ny + y
            for_ref[r] = force
            t_ref[r] = v + force
            sec_ref[r] = v + force
    rows = list(range(nx * ny))
    tiles = [rows[i : i + 2] for i in range(0, len(rows), 2)]
    newton(tiles, sec_ref, t_ref, cls_ref, rate, count, w1_ref, w2_ref, sp, deep, nclass)
    for y in range(ny):
        fx0[pl.ds(y, ns, stride=ny), :] = sec_ref[y][:ns]
        fx1[pl.ds(y, ns, stride=ny), :] = sec_ref[(nx - 1) * ny + y][:ns]
    for x in range(nx):
        fy0[pl.ds(x, ns, stride=nx), :] = sec_ref[x * ny][:ns]
        fy1[pl.ds(x, ns, stride=nx), :] = sec_ref[x * ny + ny - 1][:ns]


def last_kernel(nx, ny, ns, flags, sec_ref, for_ref, xa, xb, ya, yb, dif, out_ref, pad_ref):
    sp, nz = pad_ref.shape[2:]
    fill(pad_ref, sec_ref, flags[0], xa, xb, ya, yb, flags[1], nx, ny, ns, False)
    scale = jnp.broadcast_to(dif[...], (sp, nz))
    for x in range(nx):
        for y in range(ny):
            v, second = lap(pad_ref, x, y)
            r = x * ny + y
            value = v + 0.5 * (scale * second - for_ref[r])
            out_ref[pl.ds(r, ns, stride=nx * ny), :] = value[:ns]


def local(species, diffusion, class_rate, mixing, inverses, newton_counts, cell_class):
    ns, nx, ny, nz = species.shape
    nclass = class_rate.shape[0]
    sp, deep = up(ns, 8), up(ns, 16)
    rows = nx * ny
    even_x = lax.axis_index("gx") % 2 == 0
    even_y = lax.axis_index("gy") % 2 == 0
    flags = jnp.stack([even_x, even_y]).astype(jnp.int32)

    def face(axis, high):
        size = species.shape[axis]
        return lax.dynamic_slice_in_dim(species, jnp.where(high, size - 1, 0), 1, axis)

    xa = swap(face(1, even_x).reshape(ns * ny, nz), "gx", 0)
    xb = swap(face(1, ~even_x).reshape(ns * ny, nz), "gx", 1)
    ya = swap(face(2, even_y).reshape(ns * nx, nz), "gy", 0)
    yb = swap(face(2, ~even_y).reshape(ns * nx, nz), "gy", 1)

    w1 = packed(jnp.pad(mixing, ((0, deep - ns), (0, deep - ns))))
    scaled = (inverses * class_rate[:, None, None])[::-1]
    scaled = jnp.pad(scaled, ((0, 0), (0, sp - ns), (0, deep - ns))).reshape(nclass * sp, deep)
    w2 = packed(scaled)
    dif = jnp.pad(diffusion, (0, sp - ns))[:, None]
    classes = cell_class.reshape(rows, 1, nz)

    smem = pl.BlockSpec(memory_space=pltpu.SMEM)
    vmem = pl.BlockSpec(memory_space=pltpu.VMEM)
    row_shape = jax.ShapeDtypeStruct((rows, sp, nz), F32)
    xface = jax.ShapeDtypeStruct((ns * ny, nz), F32)
    yface = jax.ShapeDtypeStruct((ns * nx, nz), F32)
    pad = pltpu.VMEM((nx + 2, ny + 2, sp, nz), F32)
    sec, force, fx0, fx1, fy0, fy1 = pl.pallas_call(
        functools.partial(first_kernel, nx, ny, ns, nclass),
        out_shape=(row_shape, row_shape, xface, xface, yface, yface),
        in_specs=[smem] * 3 + [vmem] * 9,
        out_specs=(vmem,) * 6,
        scratch_shapes=[pad, pltpu.VMEM((rows, sp, nz), F32)],
        name="first",
    )(flags, class_rate, newton_counts, species.reshape(ns * rows, nz), xa, xb, ya, yb, dif, classes, w1, w2)

    xa = swap(jnp.where(even_x, fx1, fx0), "gx", 0)
    xb = swap(jnp.where(even_x, fx0, fx1), "gx", 1)
    ya = swap(jnp.where(even_y, fy1, fy0), "gy", 0)
    yb = swap(jnp.where(even_y, fy0, fy1), "gy", 1)
    out = pl.pallas_call(
        functools.partial(last_kernel, nx, ny, ns),
        out_shape=jax.ShapeDtypeStruct((ns * rows, nz), F32),
        in_specs=[smem] + [vmem] * 7,
        out_specs=vmem,
        scratch_shapes=[pad],
        name="last",
    )(flags, sec, force, xa, xb, ya, yb, dif)
    return out.reshape(species.shape)


def solution(mesh):
    in_specs = (P(None, "gx", "gy", None), P(), P(), P(), P(), P(), P("gx", "gy", None))
    out_specs = P(None, "gx", "gy", None)
    return jax.shard_map(local, mesh=mesh, in_specs=in_specs, out_specs=out_specs, check_vma=False)
```

```python
import functools

import jax
import jax.numpy as jnp
from jax import lax
from jax.experimental import pallas as pl
from jax.experimental.pallas import tpu as pltpu
from jax.sharding import PartitionSpec as P


F32 = jnp.float32
BF16 = jnp.bfloat16
SUB = 8
SMEM = pl.BlockSpec(memory_space=pltpu.SMEM)
VMEM = pl.BlockSpec(memory_space=pltpu.VMEM)


def up(value, step):
    return -(-value // step) * step


def swap(block, axis, first):
    count = lax.axis_size(axis)
    pairs = []
    for i in range(first, count - 1, 2):
        pairs += [(i, i + 1), (i + 1, i)]
    return lax.ppermute(block, axis, pairs)


def near_index(axis, size, inner=0):
    return jnp.where(lax.axis_index(axis) % 2 == 0, size - 1 - inner, inner)


def far_index(axis, size, inner=0):
    return jnp.where(lax.axis_index(axis) % 2 == 0, inner, size - 1 - inner)


def split(value):
    high = value.astype(BF16)
    low = (value - high.astype(F32)).astype(BF16)
    return jnp.concatenate([high, low, high], axis=0)


def widen(value, rows):
    short = rows - value.shape[0]
    if short == 0:
        return value
    return jnp.concatenate([value, jnp.zeros((short, value.shape[1]), value.dtype)], axis=0)


def put(ref, index, value, rows):
    whole = ref.shape[-2]
    if whole != rows:
        ref[(*index, slice(whole - SUB, whole), slice(None))] = jnp.zeros((SUB, ref.shape[-1]), F32)
    ref[(*index, slice(0, rows), slice(None))] = value


def newton(n, y_ref, st_ref, r1_ref, kind_ref, count, w1_ref, w2_ref, nclass):
    sp, nz = y_ref.shape[1:]
    deep = w1_ref.shape[0]
    tiles = [list(range(i, min(i + 2, n))) for i in range(0, n, 2)]

    def lanes(ref, rows):
        return jnp.concatenate([ref[r] for r in rows], axis=1)

    def tall(value):
        return jnp.concatenate([value] * (sp // SUB), axis=0)

    for low in range(nclass):
        live = nclass - low

        def body(_, carry, low=low, live=live):
            mixed = []
            for rows in tiles:
                t = widen(jnp.tanh(lanes(y_ref, rows)), deep)
                m = jnp.dot(w1_ref[...], split(t), preferred_element_type=F32)
                mixed.append(m[:sp])
            for rows, m in zip(tiles, mixed):
                y = lanes(y_ref, rows)
                g = tall(lanes(r1_ref, rows)) * y - lanes(st_ref, rows) - m
                w2 = w2_ref[: up(live * sp, 16), :]
                out = jnp.dot(w2, split(widen(g, deep)), preferred_element_type=F32)
                kind = tall(lanes(kind_ref, rows))
                step = out[(live - 1) * sp : live * sp] if low == 0 else jnp.zeros_like(y)
                for j in range(live - 1 if low == 0 else live):
                    step = jnp.where(kind == nclass - 1 - j, out[j * sp : (j + 1) * sp], step)
                y = y - step
                for i, r in enumerate(rows):
                    y_ref[r] = y[:, i * nz : (i + 1) * nz]
            return carry

        begin = 0 if low == 0 else count[low - 1]
        lax.fori_loop(begin, count[low], body, 0)


def shifted(v):
    lane = lax.broadcasted_iota(jnp.int32, v.shape, 1)
    nz = v.shape[1]
    left = jnp.where(lane == 0, 0.0, pltpu.roll(v, 1, 1))
    right = jnp.where(lane == nz - 1, 0.0, pltpu.roll(v, nz - 1, 1))
    return left + right


def lap(v, nbrs):
    total = shifted(v) - 6.0 * v
    for other in nbrs:
        total = total + other
    return total


def start_row(i, v, force, cls, rate, y_ref, st_ref, r1_ref, kind_ref, nclass):
    nz = v.shape[1]
    kind = jnp.broadcast_to(cls, (SUB, nz))
    inv = jnp.full((SUB, nz), 1.0 / rate[0], F32)
    for c in range(1, nclass):
        inv = jnp.where(kind == c, 1.0 / rate[c], inv)
    target = v + force
    y_ref[i] = target
    st_ref[i] = target * jnp.concatenate([inv] * (v.shape[0] // SUB), axis=0)
    r1_ref[i] = inv + 1.0
    kind_ref[i] = kind


def faces_kernel(nx, ny, ns, block, fa, fya, fyb):
    xa = near_index("gx", nx)
    for s in range(ns):
        fa[pl.ds(s * ny, ny), :] = block[pl.ds(s * nx * ny + xa * ny, ny), :]
    for face, y in ((fya, near_index("gy", ny)), (fyb, far_index("gy", ny))):
        for x in range(nx):
            put(face, (x,), block[pl.ds(x * ny + y, ns, stride=nx * ny), :], ns)


def inner_kernel(nx, ny, ns, nclass, rate, count, dif, block, mixing, inverses, cls,
                 s_ref, f_ref, sec, w1, w2, scale, fb,
                 y_ref, st_ref, r1_ref, kind_ref, square):
    sp, nz = s_ref.shape[2:]
    deep = square.shape[0]
    xb = far_index("gx", nx)
    for s in range(ns):
        fb[pl.ds(s * ny, ny), :] = block[pl.ds(s * nx * ny + xb * ny, ny), :]

    square[...] = jnp.zeros_like(square)

    def pack(values, rows):
        square[:ns, :ns] = values
        value = square[:rows, :]
        high = value.astype(BF16)
        back = high.astype(F32)
        return (back + pltpu.roll(back, deep, 1)).astype(BF16), (value - back).astype(BF16)[:, :deep]

    w1[:, : 2 * deep], w1[:, 2 * deep :] = pack(mixing[...], deep)
    highs, lows = [], []
    for c in reversed(range(nclass)):
        square[:ns, :ns] = inverses[c] * rate[c]
        value = square[:sp, :]
        back = value.astype(BF16).astype(F32)
        highs.append(back + pltpu.roll(back, deep, 1))
        lows.append(value - back)
    whole = w2.shape[0]
    w2[:, : 2 * deep] = widen(jnp.concatenate(highs, axis=0), whole).astype(BF16)
    w2[:, 2 * deep :] = widen(jnp.concatenate(lows, axis=0), whole).astype(BF16)[:, :deep]

    sub = lax.broadcasted_iota(jnp.int32, (SUB, nz), 0)
    for g in range(0, sp, SUB):
        value = jnp.zeros((SUB, nz), F32)
        for s in range(g, min(g + SUB, ns)):
            value = jnp.where(sub == s - g, dif[s], value)
        scale[g : g + SUB, :] = value

    for x in range(nx):
        for y in range(ny):
            put(s_ref, (x, y), block[pl.ds(x * ny + y, ns, stride=nx * ny), :], ns)
    rows = [(x, y) for x in range(1, nx - 1) for y in range(1, ny - 1)]
    for i, (x, y) in enumerate(rows):
        v = s_ref[x, y]
        force = scale[...] * lap(v, [s_ref[x - 1, y], s_ref[x + 1, y], s_ref[x, y - 1], s_ref[x, y + 1]])
        f_ref[x, y] = force
        start_row(i, v, force, cls[x, y : y + 1, :], rate, y_ref, st_ref, r1_ref, kind_ref, nclass)
    newton(len(rows), y_ref, st_ref, r1_ref, kind_ref, count, w1, w2, nclass)
    for i, (x, y) in enumerate(rows):
        sec[x, y] = y_ref[i]


def layer_rows(nx, ny, ns, near, with_edges, s_ref, halo, ya, yb):
    sp = s_ref.shape[2]
    index = near_index if near else far_index
    x0, x1 = index("gx", nx), index("gx", nx, 1)
    even_y = lax.axis_index("gy") % 2 == 0

    def edge(x, high):
        return jnp.where(even_y == high, ya[x], yb[x])

    def found(x, y, xs):
        nbrs = [get() for get in xs]
        nbrs.append(s_ref[x, y - 1] if y > 0 else edge(x, False))
        nbrs.append(s_ref[x, y + 1] if y < ny - 1 else edge(x, True))
        return x, y, s_ref[x, y], nbrs

    for y in range(ny):
        yield found(x0, y, [lambda y=y: s_ref[x1, y], lambda y=y: widen(halo[pl.ds(y, ns, stride=ny), :], sp)])
    if with_edges:
        for x in range(1, nx - 1):
            for y in (0, ny - 1):
                yield found(x, y, [lambda x=x, y=y: s_ref[x - 1, y], lambda x=x, y=y: s_ref[x + 1, y]])


def layer_kernel(nx, ny, ns, nclass, near, rate, count, s_ref, halo, ya, yb, cls, w1, w2, scale, f_in, sec_in,
                 f_ref, sec, face, *rest):
    y_ref, st_ref, r1_ref, kind_ref = rest[-4:]
    places = []
    for i, (x, y, v, nbrs) in enumerate(layer_rows(nx, ny, ns, near, near, s_ref, halo, ya, yb)):
        force = scale[...] * lap(v, nbrs)
        f_ref[x, y] = force
        start_row(i, v, force, cls[x, y : y + 1, :], rate, y_ref, st_ref, r1_ref, kind_ref, nclass)
        places.append((x, y))
    newton(len(places), y_ref, st_ref, r1_ref, kind_ref, count, w1, w2, nclass)
    for i, (x, y) in enumerate(places):
        sec[x, y] = y_ref[i]
        if i < ny:
            face[pl.ds(y, ns, stride=ny), :] = y_ref[i][:ns]
    if not near:
        fya, fyb = rest[:2]
        for out, y in ((fya, near_index("gy", ny)), (fyb, far_index("gy", ny))):
            for x in range(nx):
                out[x] = sec[x, y]


def last_kernel(nx, ny, ns, sec, f_ref, xa, xb, ya, yb, scale, out):
    sp = sec.shape[2]
    even_x = lax.axis_index("gx") % 2 == 0
    even_y = lax.axis_index("gy") % 2 == 0

    def outer(y, high):
        near = xa[pl.ds(y, ns, stride=ny), :]
        far = xb[pl.ds(y, ns, stride=ny), :]
        return widen(jnp.where(even_x == high, near, far), sp)

    for x in range(nx):
        for y in range(ny):
            v = sec[x, y]
            nbrs = [
                sec[x - 1, y] if x > 0 else outer(y, False),
                sec[x + 1, y] if x < nx - 1 else outer(y, True),
                sec[x, y - 1] if y > 0 else jnp.where(even_y == False, ya[x], yb[x]),
                sec[x, y + 1] if y < ny - 1 else jnp.where(even_y == True, ya[x], yb[x]),
            ]
            value = v + 0.5 * (scale[...] * lap(v, nbrs) - f_ref[x, y])
            out[pl.ds(x * ny + y, ns, stride=nx * ny), :] = value[:ns]


def local(species, diffusion, class_rate, mixing, inverses, newton_counts, cell_class):
    ns, nx, ny, nz = species.shape
    nclass = class_rate.shape[0]
    sp, deep = up(ns, SUB), up(ns, 16)
    block = species.reshape(ns * nx * ny, nz)
    field = jax.ShapeDtypeStruct((nx, ny, sp, nz), F32)
    xface = jax.ShapeDtypeStruct((ns * ny, nz), F32)
    yface = jax.ShapeDtypeStruct((nx, sp, nz), F32)

    def call(kernel, ins, outs, scratch=(), mib=6, work=1, alias=()):
        return pl.pallas_call(
            kernel,
            out_shape=tuple(outs),
            in_specs=[SMEM if small else VMEM for small, _ in ins],
            out_specs=(VMEM,) * len(outs),
            scratch_shapes=list(scratch),
            input_output_aliases=dict(alias),
            compiler_params=pltpu.CompilerParams(vmem_limit_bytes=mib * 2**20),
            cost_estimate=pl.CostEstimate(flops=work, bytes_accessed=1, transcendentals=0),
        )(*[value for _, value in ins])

    def scratch(n):
        return [
            pltpu.VMEM((n, sp, nz), F32),
            pltpu.VMEM((n, sp, nz), F32),
            pltpu.VMEM((n, SUB, nz), F32),
            pltpu.VMEM((n, SUB, nz), jnp.int32),
        ]

    big = lambda *values: [(False, v) for v in values]
    small = lambda *values: [(True, v) for v in values]
    us = 10**9

    fa, fya, fyb = call(functools.partial(faces_kernel, nx, ny, ns), big(block), [xface, yface, yface], work=us // 2)
    ha = swap(fa, "gx", 0)
    hya = swap(fya, "gy", 0)
    hyb = swap(fyb, "gy", 1)

    s_ref, force, sec, w1, w2, scale, fb = call(
        functools.partial(inner_kernel, nx, ny, ns, nclass),
        small(class_rate, newton_counts, diffusion) + big(block, mixing, inverses, cell_class),
        [
            field,
            field,
            field,
            jax.ShapeDtypeStruct((deep, 3 * deep), BF16),
            jax.ShapeDtypeStruct((up(nclass * sp, 16), 3 * deep), BF16),
            jax.ShapeDtypeStruct((sp, nz), F32),
            xface,
        ],
        scratch((nx - 2) * (ny - 2)) + [pltpu.VMEM((deep, 2 * deep), F32)],
        mib=10,
        work=4 * us,
    )
    hb = swap(fb, "gx", 1)

    def layer(near, halo, force, sec):
        n = ny + (2 * (nx - 2) if near else 0)
        ins = small(class_rate, newton_counts) + big(s_ref, halo, hya, hyb, cell_class, w1, w2, scale, force, sec)
        outs = [field, field, xface] + ([] if near else [yface, yface])
        kernel = functools.partial(layer_kernel, nx, ny, ns, nclass, near)
        return call(kernel, ins, outs, scratch(n), mib=10, work=4 * us, alias=((10, 0), (11, 1)))

    force, sec, fa = layer(True, ha, force, sec)
    ha = swap(fa, "gx", 0)
    force, sec, fb, fya, fyb = layer(False, hb, force, sec)
    hb = swap(fb, "gx", 1)
    hya = swap(fya, "gy", 0)
    hyb = swap(fyb, "gy", 1)
    (out,) = call(
        functools.partial(last_kernel, nx, ny, ns),
        big(sec, force, ha, hb, hya, hyb, scale),
        [jax.ShapeDtypeStruct(block.shape, F32)],
        work=2 * us,
    )
    return out.reshape(species.shape)


def solution(mesh):
    in_specs = (P(None, "gx", "gy", None), P(), P(), P(), P(), P(), P("gx", "gy", None))
    out_specs = P(None, "gx", "gy", None)


    return jax.shard_map(local, mesh=mesh, in_specs=in_specs, out_specs=out_specs, check_vma=False)
```

```python
import functools

import jax
import jax.numpy as jnp
from jax import lax
from jax.experimental import pallas as pl
from jax.experimental.pallas import tpu as pltpu
from jax.sharding import PartitionSpec as P


F32 = jnp.float32
BF16 = jnp.bfloat16
SUB = 8
SMEM = pl.BlockSpec(memory_space=pltpu.SMEM)
VMEM = pl.BlockSpec(memory_space=pltpu.VMEM)


def up(value, step):
    return -(-value // step) * step


def swap(block, axis, first):
    count = lax.axis_size(axis)
    pairs = []
    for i in range(first, count - 1, 2):
        pairs += [(i, i + 1), (i + 1, i)]
    return lax.ppermute(block, axis, pairs)


def near_index(axis, size, inner=0):
    return jnp.where(lax.axis_index(axis) % 2 == 0, size - 1 - inner, inner)


def far_index(axis, size, inner=0):
    return jnp.where(lax.axis_index(axis) % 2 == 0, inner, size - 1 - inner)


def split(value):
    high = value.astype(BF16)
    low = (value - high.astype(F32)).astype(BF16)
    return jnp.concatenate([high, low, high], axis=0)


def widen(value, rows):
    short = rows - value.shape[0]
    if short == 0:
        return value
    return jnp.concatenate([value, jnp.zeros((short, value.shape[1]), value.dtype)], axis=0)


def put(ref, index, value, rows):
    whole = ref.shape[-2]
    if whole != rows:
        ref[(*index, slice(whole - SUB, whole), slice(None))] = jnp.zeros((SUB, ref.shape[-1]), F32)
    ref[(*index, slice(0, rows), slice(None))] = value


def newton(n, y_ref, st_ref, r1_ref, kind_ref, count, w1_ref, w2_ref, nclass):
    sp, nz = y_ref.shape[1:]
    deep = w1_ref.shape[0]
    tiles = [list(range(i, min(i + 2, n))) for i in range(0, n, 2)]

    def lanes(ref, rows):
        return jnp.concatenate([ref[r] for r in rows], axis=1)

    def tall(value):
        return jnp.concatenate([value] * (sp // SUB), axis=0)

    for low in range(nclass):
        live = nclass - low

        def body(_, carry, low=low, live=live):
            mixed = []
            for rows in tiles:
                t = widen(jnp.tanh(lanes(y_ref, rows)), deep)
                m = jnp.dot(w1_ref[...], split(t), preferred_element_type=F32)
                mixed.append(m[:sp])
            for rows, m in zip(tiles, mixed):
                y = lanes(y_ref, rows)
                g = tall(lanes(r1_ref, rows)) * y - lanes(st_ref, rows) - m
                w2 = w2_ref[: up(live * sp, 16), :]
                out = jnp.dot(w2, split(widen(g, deep)), preferred_element_type=F32)
                kind = tall(lanes(kind_ref, rows))
                step = out[(live - 1) * sp : live * sp] if low == 0 else jnp.zeros_like(y)
                for j in range(live - 1 if low == 0 else live):
                    step = jnp.where(kind == nclass - 1 - j, out[j * sp : (j + 1) * sp], step)
                y = y - step
                for i, r in enumerate(rows):
                    y_ref[r] = y[:, i * nz : (i + 1) * nz]
            return carry

        begin = 0 if low == 0 else count[low - 1]
        lax.fori_loop(begin, count[low], body, 0)


def shifted(v):
    lane = lax.broadcasted_iota(jnp.int32, v.shape, 1)
    nz = v.shape[1]
    left = jnp.where(lane == 0, 0.0, pltpu.roll(v, 1, 1))
    right = jnp.where(lane == nz - 1, 0.0, pltpu.roll(v, nz - 1, 1))
    return left + right


def lap(v, nbrs):
    total = shifted(v) - 6.0 * v
    for other in nbrs:
        total = total + other
    return total


def start_row(i, target, cls, rate, y_ref, st_ref, r1_ref, kind_ref, nclass):
    sp, nz = target.shape
    kind = jnp.broadcast_to(cls, (SUB, nz))
    inv = jnp.full((SUB, nz), 1.0 / rate[0], F32)
    for c in range(1, nclass):
        inv = jnp.where(kind == c, 1.0 / rate[c], inv)
    y_ref[i] = target
    st_ref[i] = target * jnp.concatenate([inv] * (sp // SUB), axis=0)
    r1_ref[i] = inv + 1.0
    kind_ref[i] = kind


def faces_kernel(nx, ny, ns, block, fa, fya, fyb):
    xa = near_index("gx", nx)
    for s in range(ns):
        fa[pl.ds(s * ny, ny), :] = block[pl.ds(s * nx * ny + xa * ny, ny), :]
    for face, y in ((fya, near_index("gy", ny)), (fyb, far_index("gy", ny))):
        for x in range(nx):
            put(face, (x,), block[pl.ds(x * ny + y, ns, stride=nx * ny), :], ns)


def make_scale(scale, dif, ns):
    sp, nz = scale.shape
    sub = lax.broadcasted_iota(jnp.int32, (SUB, nz), 0)
    for g in range(0, sp, SUB):
        value = jnp.zeros((SUB, nz), F32)
        for s in range(g, min(g + SUB, ns)):
            value = jnp.where(sub == s - g, dif[s], value)
        scale[g : g + SUB, :] = value


def make_weights(w1, w2, square, mixing, inverses, rate, ns, sp, nclass):
    deep = square.shape[0]
    square[...] = jnp.zeros_like(square)
    square[:ns, :ns] = mixing[...]
    value = square[...]
    back = value.astype(BF16).astype(F32)
    w1[:, : 2 * deep] = (back + pltpu.roll(back, deep, 1)).astype(BF16)
    w1[:, 2 * deep :] = (value - back).astype(BF16)[:, :deep]
    highs, lows = [], []
    for c in reversed(range(nclass)):
        square[:ns, :ns] = inverses[c] * rate[c]
        value = square[:sp, :]
        back = value.astype(BF16).astype(F32)
        highs.append(back + pltpu.roll(back, deep, 1))
        lows.append(value - back)
    whole = w2.shape[0]
    w2[:, : 2 * deep] = widen(jnp.concatenate(highs, axis=0), whole).astype(BF16)
    w2[:, 2 * deep :] = widen(jnp.concatenate(lows, axis=0), whole).astype(BF16)[:, :deep]


def edge_rows(ya, yb):
    even_y = lax.axis_index("gy") % 2 == 0
    return lambda x, high: jnp.where(even_y == high, ya[x], yb[x])


def send_kernel(nx, ny, ns, dif, block, ya, yb, cls, s_ref, scale, message):
    make_scale(scale, dif, ns)
    far, inner = far_index("gx", nx), far_index("gx", nx, 1)
    edge = edge_rows(ya, yb)
    for x in range(nx):
        for y in range(ny):
            put(s_ref, (x, y), block[pl.ds(x * ny + y, ns, stride=nx * ny), :], ns)
    for s in range(ns):
        message[pl.ds(s * ny, ny), :] = block[pl.ds(s * nx * ny + far * ny, ny), :]
    for y in range(ny):
        v = s_ref[far, y]
        low = s_ref[far, y - 1] if y > 0 else edge(far, False)
        high = s_ref[far, y + 1] if y < ny - 1 else edge(far, True)
        part = v + scale[...] * lap(v, [s_ref[inner, y], low, high])
        message[pl.ds(ns * ny + y, ns, stride=ny), :] = part[:ns]
    message[pl.ds(2 * ns * ny, ny), :] = cls[far].astype(F32)


def near_kernel(nx, ny, ns, nclass, rate, count, s_ref, halo, ya, yb, mixing, inverses, cls, scale,
                f_ref, sec, face, w1, w2, y_ref, st_ref, r1_ref, kind_ref, square):
    sp = s_ref.shape[2]
    make_weights(w1, w2, square, mixing, inverses, rate, ns, sp, nclass)
    edge = edge_rows(ya, yb)
    near, inner = near_index("gx", nx), near_index("gx", nx, 1)
    places = [(near, y) for y in range(ny)] + [(x, y) for x in range(1, nx - 1) for y in range(ny)]
    for i, (x, y) in enumerate(places):
        if i < ny:
            nbrs = [s_ref[inner, y], widen(halo[pl.ds(y, ns, stride=ny), :], sp)]
        else:
            nbrs = [s_ref[x - 1, y], s_ref[x + 1, y]]
        nbrs.append(s_ref[x, y - 1] if y > 0 else edge(x, False))
        nbrs.append(s_ref[x, y + 1] if y < ny - 1 else edge(x, True))
        v = s_ref[x, y]
        force = scale[...] * lap(v, nbrs)
        f_ref[x, y] = force
        start_row(i, v + force, cls[x, y : y + 1, :], rate, y_ref, st_ref, r1_ref, kind_ref, nclass)
    newton(len(places), y_ref, st_ref, r1_ref, kind_ref, count, w1, w2, nclass)
    for i, (x, y) in enumerate(places):
        sec[x, y] = y_ref[i]
        if i < ny:
            face[pl.ds(y, ns, stride=ny), :] = y_ref[i][:ns]


def far_kernel(nx, ny, ns, nclass, rate, count, s_ref, message, ya, yb, cls, scale, w1, w2, f_in, sec_in,
               f_ref, sec, beyond, fya, fyb, y_ref, st_ref, r1_ref, kind_ref):
    sp = s_ref.shape[2]
    edge = edge_rows(ya, yb)
    far, inner = far_index("gx", nx), far_index("gx", nx, 1)
    me, last = lax.axis_index("gx"), lax.axis_size("gx") - 1
    has = jnp.where(me % 2 == 0, me > 0, me < last)
    for y in range(ny):
        v = s_ref[far, y]
        nbrs = [
            s_ref[inner, y],
            widen(message[pl.ds(y, ns, stride=ny), :], sp),
            s_ref[far, y - 1] if y > 0 else edge(far, False),
            s_ref[far, y + 1] if y < ny - 1 else edge(far, True),
        ]
        force = scale[...] * lap(v, nbrs)
        f_ref[far, y] = force
        start_row(y, v + force, cls[far, y : y + 1, :], rate, y_ref, st_ref, r1_ref, kind_ref, nclass)
        target = widen(message[pl.ds(ns * ny + y, ns, stride=ny), :], sp) + scale[...] * v
        kind = message[pl.ds(2 * ns * ny + y, 1), :].astype(jnp.int32)
        start_row(ny + y, target, kind, rate, y_ref, st_ref, r1_ref, kind_ref, nclass)
    newton(2 * ny, y_ref, st_ref, r1_ref, kind_ref, count, w1, w2, nclass)
    for y in range(ny):
        sec[far, y] = y_ref[y]
        beyond[y] = jnp.where(has, y_ref[ny + y], 0.0)
    for out, y in ((fya, near_index("gy", ny)), (fyb, far_index("gy", ny))):
        for x in range(nx):
            out[x] = sec[x, y]


def last_kernel(nx, ny, ns, sec, f_ref, xa, beyond, ya, yb, scale, out):
    sp = sec.shape[2]
    even_x = lax.axis_index("gx") % 2 == 0
    edge = edge_rows(ya, yb)

    def outer(y, high):
        near = widen(xa[pl.ds(y, ns, stride=ny), :], sp)
        return jnp.where(even_x == high, near, beyond[y])

    for x in range(nx):
        for y in range(ny):
            v = sec[x, y]
            nbrs = [
                sec[x - 1, y] if x > 0 else outer(y, False),
                sec[x + 1, y] if x < nx - 1 else outer(y, True),
                sec[x, y - 1] if y > 0 else edge(x, False),
                sec[x, y + 1] if y < ny - 1 else edge(x, True),
            ]
            value = v + 0.5 * (scale[...] * lap(v, nbrs) - f_ref[x, y])
            out[pl.ds(x * ny + y, ns, stride=nx * ny), :] = value[:ns]


def local(species, diffusion, class_rate, mixing, inverses, newton_counts, cell_class):
    ns, nx, ny, nz = species.shape
    nclass = class_rate.shape[0]
    sp, deep = up(ns, SUB), up(ns, 16)
    block = species.reshape(ns * nx * ny, nz)

    def shape(*dims, dtype=F32):
        return jax.ShapeDtypeStruct(dims, dtype)

    field = shape(nx, ny, sp, nz)
    xface = shape(ns * ny, nz)
    yface = shape(nx, sp, nz)

    def call(kernel, small, big, outs, scratch=(), mib=6, work=1, alias=()):
        return pl.pallas_call(
            kernel,
            out_shape=tuple(outs),
            in_specs=[SMEM] * len(small) + [VMEM] * len(big),
            out_specs=(VMEM,) * len(outs),
            scratch_shapes=list(scratch),
            input_output_aliases=dict(alias),
            compiler_params=pltpu.CompilerParams(vmem_limit_bytes=mib * 2**20),
            cost_estimate=pl.CostEstimate(flops=work, bytes_accessed=1, transcendentals=0),
        )(*small, *big)

    def scratch(n):
        return [
            pltpu.VMEM((n, sp, nz), F32),
            pltpu.VMEM((n, sp, nz), F32),
            pltpu.VMEM((n, SUB, nz), F32),
            pltpu.VMEM((n, SUB, nz), jnp.int32),
        ]

    us = 10**9
    fa, fya, fyb = call(functools.partial(faces_kernel, nx, ny, ns), [], [block], [xface, yface, yface])
    ha = swap(fa, "gx", 0)
    hya = swap(fya, "gy", 0)
    hyb = swap(fyb, "gy", 1)
    s_ref, scale, message = call(
        functools.partial(send_kernel, nx, ny, ns),
        [diffusion],
        [block, hya, hyb, cell_class],
        [field, shape(sp, nz), shape(2 * ns * ny + ny, nz)],
        work=us,
    )
    message = swap(message, "gx", 1)
    force, sec, fa, w1, w2 = call(
        functools.partial(near_kernel, nx, ny, ns, nclass),
        [class_rate, newton_counts],
        [s_ref, ha, hya, hyb, mixing, inverses, cell_class, scale],
        [field, field, xface, shape(deep, 3 * deep, dtype=BF16), shape(up(nclass * sp, 16), 3 * deep, dtype=BF16)],
        scratch((nx - 1) * ny) + [pltpu.VMEM((deep, 2 * deep), F32)],
        mib=14,
        work=6 * us,
    )
    ha = swap(fa, "gx", 0)
    force, sec, beyond, fya, fyb = call(
        functools.partial(far_kernel, nx, ny, ns, nclass),
        [class_rate, newton_counts],
        [s_ref, message, hya, hyb, cell_class, scale, w1, w2, force, sec],
        [field, field, shape(ny, sp, nz), yface, yface],
        scratch(2 * ny),
        mib=12,
        work=4 * us,
        alias=((10, 0), (11, 1)),
    )
    hya = swap(fya, "gy", 0)
    hyb = swap(fyb, "gy", 1)
    (out,) = call(
        functools.partial(last_kernel, nx, ny, ns),
        [],
        [sec, force, ha, beyond, hya, hyb, scale],
        [shape(*block.shape)],
        work=2 * us,
    )
    return out.reshape(species.shape)


def solution(mesh):
    in_specs = (P(None, "gx", "gy", None), P(), P(), P(), P(), P(), P("gx", "gy", None))
    out_specs = P(None, "gx", "gy", None)


    return jax.shard_map(local, mesh=mesh, in_specs=in_specs, out_specs=out_specs, check_vma=False)
```

```python
import functools

import jax
import jax.numpy as jnp
from jax import lax
from jax.experimental import pallas as pl
from jax.experimental.pallas import tpu as pltpu
from jax.sharding import PartitionSpec as P


F32 = jnp.float32
BF16 = jnp.bfloat16
SUB = 8
SMEM = pl.BlockSpec(memory_space=pltpu.SMEM)
VMEM = pl.BlockSpec(memory_space=pltpu.VMEM)


def up(value, step):
    return -(-value // step) * step


def swap(block, axis, first):
    count = lax.axis_size(axis)
    pairs = []
    for i in range(first, count - 1, 2):
        pairs += [(i, i + 1), (i + 1, i)]
    return lax.ppermute(block, axis, pairs)


def hand_on(block, axis):
    count = lax.axis_size(axis)
    pairs = [(i, i + 2) for i in range(0, count - 2, 2)] + [(i, i - 2) for i in range(3, count, 2)]
    return lax.ppermute(block, axis, pairs)


def near_index(axis, size, inner=0):
    return jnp.where(lax.axis_index(axis) % 2 == 0, size - 1 - inner, inner)


def far_index(axis, size, inner=0):
    return jnp.where(lax.axis_index(axis) % 2 == 0, inner, size - 1 - inner)


def split(value):
    high = value.astype(BF16)
    low = (value - high.astype(F32)).astype(BF16)
    return jnp.concatenate([high, low, high], axis=0)


def widen(value, rows):
    short = rows - value.shape[0]
    if short == 0:
        return value
    return jnp.concatenate([value, jnp.zeros((short, value.shape[1]), value.dtype)], axis=0)


def put(ref, index, value, rows):
    whole = ref.shape[-2]
    if whole != rows:
        ref[(*index, slice(whole - SUB, whole), slice(None))] = jnp.zeros((SUB, ref.shape[-1]), F32)
    ref[(*index, slice(0, rows), slice(None))] = value


def newton(n, y_ref, st_ref, r1_ref, kind_ref, count, w1_ref, w2_ref, nclass):
    sp, nz = y_ref.shape[1:]
    deep = w1_ref.shape[0]
    tiles = [list(range(i, min(i + 2, n))) for i in range(0, n, 2)]

    def lanes(ref, rows):
        return jnp.concatenate([ref[r] for r in rows], axis=1)

    def tall(value):
        return jnp.concatenate([value] * (sp // SUB), axis=0)

    for low in range(nclass):
        live = nclass - low

        def body(_, carry, low=low, live=live):
            mixed = []
            for rows in tiles:
                t = widen(jnp.tanh(lanes(y_ref, rows)), deep)
                m = jnp.dot(w1_ref[...], split(t), preferred_element_type=F32)
                mixed.append(m[:sp])
            for rows, m in zip(tiles, mixed):
                y = lanes(y_ref, rows)
                g = tall(lanes(r1_ref, rows)) * y - lanes(st_ref, rows) - m
                w2 = w2_ref[: up(live * sp, 16), :]
                out = jnp.dot(w2, split(widen(g, deep)), preferred_element_type=F32)
                kind = tall(lanes(kind_ref, rows))
                step = out[(live - 1) * sp : live * sp] if low == 0 else jnp.zeros_like(y)
                for j in range(live - 1 if low == 0 else live):
                    step = jnp.where(kind == nclass - 1 - j, out[j * sp : (j + 1) * sp], step)
                y = y - step
                for i, r in enumerate(rows):
                    y_ref[r] = y[:, i * nz : (i + 1) * nz]
            return carry

        begin = 0 if low == 0 else count[low - 1]
        lax.fori_loop(begin, count[low], body, 0)


def shifted(v):
    lane = lax.broadcasted_iota(jnp.int32, v.shape, 1)
    nz = v.shape[1]
    left = jnp.where(lane == 0, 0.0, pltpu.roll(v, 1, 1))
    right = jnp.where(lane == nz - 1, 0.0, pltpu.roll(v, nz - 1, 1))
    return left + right


def lap(v, nbrs):
    total = shifted(v) - 6.0 * v
    for other in nbrs:
        total = total + other
    return total


def start_row(i, target, cls, rate, y_ref, st_ref, r1_ref, kind_ref, nclass):
    sp, nz = target.shape
    kind = jnp.broadcast_to(cls, (SUB, nz))
    inv = jnp.full((SUB, nz), 1.0 / rate[0], F32)
    for c in range(1, nclass):
        inv = jnp.where(kind == c, 1.0 / rate[c], inv)
    y_ref[i] = target
    st_ref[i] = target * jnp.concatenate([inv] * (sp // SUB), axis=0)
    r1_ref[i] = inv + 1.0
    kind_ref[i] = kind


def exists(axis):
    me, last = lax.axis_index(axis), lax.axis_size(axis) - 1
    return jnp.where(me % 2 == 0, me > 0, me < last)


def faces_kernel(nx, ny, ns, rate, count, dif, block, cls, mixing, fa, fy):
    xa, far = near_index("gx", nx), far_index("gx", nx)
    for s in range(ns):
        fa[pl.ds(s * ny, ny), :] = block[pl.ds(s * nx * ny + xa * ny, ny), :]
    for k, index in enumerate((near_index, far_index)):
        y, inner = index("gy", ny), index("gy", ny, 1)
        first = k * (nx + 1)
        for x in range(nx):
            put(fy, (first + x,), block[pl.ds(x * ny + y, ns, stride=nx * ny), :], ns)
        put(fy, (first + nx,), block[pl.ds(far * ny + inner, ns, stride=nx * ny), :], ns)
        fy[first + nx, ns : ns + 1, :] = cls[far, pl.ds(y, 1), :].astype(F32)


def make_scale(scale, dif, ns):
    sp, nz = scale.shape
    sub = lax.broadcasted_iota(jnp.int32, (SUB, nz), 0)
    for g in range(0, sp, SUB):
        value = jnp.zeros((SUB, nz), F32)
        for s in range(g, min(g + SUB, ns)):
            value = jnp.where(sub == s - g, dif[s], value)
        scale[g : g + SUB, :] = value


def make_weights(w1, w2, square, mixing, inverses, rate, ns, sp, nclass):
    deep = square.shape[0]
    square[...] = jnp.zeros_like(square)
    square[:ns, :ns] = mixing[...]
    value = square[...]
    back = value.astype(BF16).astype(F32)
    w1[:, : 2 * deep] = (back + pltpu.roll(back, deep, 1)).astype(BF16)
    w1[:, 2 * deep :] = (value - back).astype(BF16)[:, :deep]
    highs, lows = [], []
    for c in reversed(range(nclass)):
        square[:ns, :ns] = inverses[c] * rate[c]
        value = square[:sp, :]
        back = value.astype(BF16).astype(F32)
        highs.append(back + pltpu.roll(back, deep, 1))
        lows.append(value - back)
    whole = w2.shape[0]
    w2[:, : 2 * deep] = widen(jnp.concatenate(highs, axis=0), whole).astype(BF16)
    w2[:, 2 * deep :] = widen(jnp.concatenate(lows, axis=0), whole).astype(BF16)[:, :deep]


def prep_kernel(nx, ny, ns, nclass, rate, dif, block, mixing, inverses, s_ref, scale, w1, w2, square):
    make_scale(scale, dif, ns)
    make_weights(w1, w2, square, mixing, inverses, rate, ns, s_ref.shape[2], nclass)
    for x in range(nx):
        for y in range(ny):
            put(s_ref, (x, y), block[pl.ds(x * ny + y, ns, stride=nx * ny), :], ns)


def edge_rows(ya, yb):
    even_y = lax.axis_index("gy") % 2 == 0
    return lambda x, high: jnp.where(even_y == high, ya[x], yb[x])


def send_kernel(nx, ny, ns, block, s_ref, ya, yb, cls, scale, message):
    far, inner = far_index("gx", nx), far_index("gx", nx, 1)
    edge = edge_rows(ya, yb)
    for s in range(ns):
        message[pl.ds(s * ny, ny), :] = block[pl.ds(s * nx * ny + far * ny, ny), :]
    for y in range(ny):
        v = s_ref[far, y]
        low = s_ref[far, y - 1] if y > 0 else edge(far, False)
        high = s_ref[far, y + 1] if y < ny - 1 else edge(far, True)
        part = v + scale[...] * lap(v, [s_ref[inner, y], low, high])
        message[pl.ds(ns * ny + y, ns, stride=ny), :] = part[:ns]
    base = 2 * ns * ny
    message[pl.ds(base, ny), :] = cls[far].astype(F32)
    message[pl.ds(base + ny, ns, stride=2), :] = ya[far][:ns]
    message[pl.ds(base + ny + 1, ns, stride=2), :] = yb[far][:ns]


def near_kernel(nx, ny, ns, nclass, rate, count, s_ref, halo, ya, yb, cls, scale, w1, w2,
                f_ref, sec, face, fy, y_ref, st_ref, r1_ref, kind_ref):
    sp, nz = s_ref.shape[2:]
    edge = edge_rows(ya, yb)
    near, inner, far = near_index("gx", nx), near_index("gx", nx, 1), far_index("gx", nx)
    places = [(near, y) for y in range(ny)] + [(x, y) for x in range(1, nx - 1) for y in range(ny)]
    for i, (x, y) in enumerate(places):
        if i < ny:
            nbrs = [s_ref[inner, y], widen(halo[pl.ds(y, ns, stride=ny), :], sp)]
        else:
            nbrs = [s_ref[x - 1, y], s_ref[x + 1, y]]
        nbrs.append(s_ref[x, y - 1] if y > 0 else edge(x, False))
        nbrs.append(s_ref[x, y + 1] if y < ny - 1 else edge(x, True))
        v = s_ref[x, y]
        force = scale[...] * lap(v, nbrs)
        f_ref[x, y] = force
        start_row(i, v + force, cls[x, y : y + 1, :], rate, y_ref, st_ref, r1_ref, kind_ref, nclass)
    newton(len(places), y_ref, st_ref, r1_ref, kind_ref, count, w1, w2, nclass)
    for i, (x, y) in enumerate(places):
        sec[x, y] = y_ref[i]
        if i < ny:
            face[pl.ds(y, ns, stride=ny), :] = y_ref[i][:ns]
    for k, y in enumerate((near_index("gy", ny), far_index("gy", ny))):
        fy[k * nx + far] = jnp.zeros((sp, nz), F32)
        fy[k * nx + near] = sec[near, y]
        for x in range(1, nx - 1):
            fy[k * nx + x] = sec[x, y]


def far_kernel(nx, ny, ns, nclass, rate, count, s_ref, message, ya, yb, cls, scale, w1, w2, f_in, sec_in,
               f_ref, sec, beyond, beside, y_ref, st_ref, r1_ref, kind_ref):
    sp = s_ref.shape[2]
    edge = edge_rows(ya, yb)
    far, inner = far_index("gx", nx), far_index("gx", nx, 1)
    base = 2 * ns * ny

    def begin(i, target, kind):
        start_row(i, target, kind, rate, y_ref, st_ref, r1_ref, kind_ref, nclass)

    for y in range(ny):
        v = s_ref[far, y]
        nbrs = [
            s_ref[inner, y],
            widen(message[pl.ds(y, ns, stride=ny), :], sp),
            s_ref[far, y - 1] if y > 0 else edge(far, False),
            s_ref[far, y + 1] if y < ny - 1 else edge(far, True),
        ]
        force = scale[...] * lap(v, nbrs)
        f_ref[far, y] = force
        begin(y, v + force, cls[far, y : y + 1, :])
        target = widen(message[pl.ds(ns * ny + y, ns, stride=ny), :], sp) + scale[...] * v
        begin(ny + y, target, message[pl.ds(base + y, 1), :].astype(jnp.int32))
    for k, (halo, y) in enumerate(((ya, near_index("gy", ny)), (yb, far_index("gy", ny)))):
        v = halo[far]
        corner = widen(message[pl.ds(base + ny + k, ns, stride=2), :], sp)
        target = v + scale[...] * lap(v, [halo[inner], corner, halo[nx], s_ref[far, y]])
        begin(2 * ny + k, target, halo[nx, ns : ns + 1, :].astype(jnp.int32))
    newton(2 * ny + 2, y_ref, st_ref, r1_ref, kind_ref, count, w1, w2, nclass)
    there = exists("gx")
    for y in range(ny):
        sec[far, y] = y_ref[y]
        beyond[y] = jnp.where(there, y_ref[ny + y], 0.0)
    beside[0] = y_ref[2 * ny]
    beside[1] = jnp.where(exists("gy"), y_ref[2 * ny + 1], 0.0)


def last_kernel(nx, ny, ns, sec, f_ref, xa, beyond, ya, yb, beside, scale, out):
    sp = sec.shape[2]
    even_x = lax.axis_index("gx") % 2 == 0
    even_y = lax.axis_index("gy") % 2 == 0

    def outer(y, high):
        near = widen(xa[pl.ds(y, ns, stride=ny), :], sp)
        return jnp.where(even_x == high, near, beyond[y])

    def edge(x, high):
        value = jnp.where(even_y == high, ya[x], yb[x])
        if 0 < x < nx - 1:
            return value
        side = jnp.where(even_y == high, beside[0], beside[1])
        return jnp.where(even_x == (x == 0), side, value)

    for x in range(nx):
        for y in range(ny):
            v = sec[x, y]
            nbrs = [
                sec[x - 1, y] if x > 0 else outer(y, False),
                sec[x + 1, y] if x < nx - 1 else outer(y, True),
                sec[x, y - 1] if y > 0 else edge(x, False),
                sec[x, y + 1] if y < ny - 1 else edge(x, True),
            ]
            value = v + 0.5 * (scale[...] * lap(v, nbrs) - f_ref[x, y])
            out[pl.ds(x * ny + y, ns, stride=nx * ny), :] = value[:ns]


def local(species, diffusion, class_rate, mixing, inverses, newton_counts, cell_class):
    ns, nx, ny, nz = species.shape
    nclass = class_rate.shape[0]
    sp = up(ns + 1, SUB)
    deep = up(sp, 16)
    block = species.reshape(ns * nx * ny, nz)

    def shape(*dims, dtype=F32):
        return jax.ShapeDtypeStruct(dims, dtype)

    field = shape(nx, ny, sp, nz)
    xface = shape(ns * ny, nz)

    def call(kernel, small, big, outs, scratch=(), mib=6, work=1, alias=()):
        return pl.pallas_call(
            kernel,
            out_shape=tuple(outs),
            in_specs=[SMEM] * len(small) + [VMEM] * len(big),
            out_specs=(VMEM,) * len(outs),
            scratch_shapes=list(scratch),
            input_output_aliases=dict(alias),
            compiler_params=pltpu.CompilerParams(vmem_limit_bytes=mib * 2**20),
            cost_estimate=pl.CostEstimate(flops=work, bytes_accessed=1, transcendentals=0),
        )(*small, *big)

    def scratch(n):
        return [
            pltpu.VMEM((n, sp, nz), F32),
            pltpu.VMEM((n, sp, nz), F32),
            pltpu.VMEM((n, SUB, nz), F32),
            pltpu.VMEM((n, SUB, nz), jnp.int32),
        ]

    us = 10**9
    part = functools.partial
    rate, count = class_rate, newton_counts
    fa, fy = call(
        part(faces_kernel, nx, ny, ns),
        [rate, count, diffusion],
        [block, cell_class, mixing],
        [xface, shape(2 * (nx + 1), sp, nz)],
    )
    hya = swap(fy, "gy", 0)
    ha = swap(fa, "gx", 0)
    hyb = hand_on(hya[nx + 1 :], "gy")
    s_ref, scale, w1, w2 = call(
        part(prep_kernel, nx, ny, ns, nclass),
        [rate, diffusion],
        [block, mixing, inverses],
        [field, shape(sp, nz), shape(deep, 3 * deep, dtype=BF16), shape(up(nclass * sp, 16), 3 * deep, dtype=BF16)],
        [pltpu.VMEM((deep, 2 * deep), F32)],
        work=us,
    )
    (message,) = call(
        part(send_kernel, nx, ny, ns),
        [],
        [block, s_ref, hya, hyb, cell_class, scale],
        [shape(2 * ns * ny + ny + 2 * ns, nz)],
        work=us // 2,
    )
    message = swap(message, "gx", 1)
    force, sec, fa, fy = call(
        part(near_kernel, nx, ny, ns, nclass),
        [rate, count],
        [s_ref, ha, hya, hyb, cell_class, scale, w1, w2],
        [field, field, xface, shape(2 * nx, sp, nz)],
        scratch((nx - 1) * ny),
        mib=14,
        work=6 * us,
    )
    back_ya = swap(fy, "gy", 0)
    ha = swap(fa, "gx", 0)
    back_yb = hand_on(back_ya[nx:], "gy")
    force, sec, beyond, beside = call(
        part(far_kernel, nx, ny, ns, nclass),
        [rate, count],
        [s_ref, message, hya, hyb, cell_class, scale, w1, w2, force, sec],
        [field, field, shape(ny, sp, nz), shape(2, sp, nz)],
        scratch(2 * ny + 2),
        mib=12,
        work=5 * us,
        alias=((10, 0), (11, 1)),
    )
    (out,) = call(
        part(last_kernel, nx, ny, ns),
        [],
        [sec, force, ha, beyond, back_ya, back_yb, beside, scale],
        [shape(*block.shape)],
        work=2 * us,
    )
    return out.reshape(species.shape)


def solution(mesh):
    in_specs = (P(None, "gx", "gy", None), P(), P(), P(), P(), P(), P("gx", "gy", None))
    out_specs = P(None, "gx", "gy", None)


    return jax.shard_map(local, mesh=mesh, in_specs=in_specs, out_specs=out_specs, check_vma=False)
```

```python
import functools

import jax
import jax.numpy as jnp
from jax import lax
from jax.experimental import pallas as pl
from jax.experimental.pallas import tpu as pltpu
from jax.sharding import PartitionSpec as P


F32 = jnp.float32
BF16 = jnp.bfloat16
SUB = 8
SMEM = pl.BlockSpec(memory_space=pltpu.SMEM)
VMEM = pl.BlockSpec(memory_space=pltpu.VMEM)


def up(value, step):
    return -(-value // step) * step


def swap(block, axis, first):
    count = lax.axis_size(axis)
    pairs = []
    for i in range(first, count - 1, 2):
        pairs += [(i, i + 1), (i + 1, i)]
    return lax.ppermute(block, axis, pairs)


def near_index(axis, size, inner=0):
    return jnp.where(lax.axis_index(axis) % 2 == 0, size - 1 - inner, inner)


def far_index(axis, size, inner=0):
    return jnp.where(lax.axis_index(axis) % 2 == 0, inner, size - 1 - inner)


def split(value):
    high = value.astype(BF16)
    low = (value - high.astype(F32)).astype(BF16)
    return jnp.concatenate([high, low, high], axis=0)


def widen(value, rows):
    short = rows - value.shape[0]
    if short == 0:
        return value
    return jnp.concatenate([value, jnp.zeros((short, value.shape[1]), value.dtype)], axis=0)


def put(ref, index, value, rows):
    whole = ref.shape[-2]
    if whole != rows:
        ref[(*index, slice(whole - SUB, whole), slice(None))] = jnp.zeros((SUB, ref.shape[-1]), F32)
    ref[(*index, slice(0, rows), slice(None))] = value


def newton(n, y_ref, st_ref, r1_ref, kind_ref, counts, w1_ref, w2_ref, nclass):
    sp, nz = y_ref.shape[1:]
    deep = w1_ref.shape[0]
    tiles = [list(range(i, min(i + 2, n))) for i in range(0, n, 2)]

    def lanes(ref, rows):
        return jnp.concatenate([ref[r] for r in rows], axis=1)

    def tall(value):
        return jnp.concatenate([value] * (sp // SUB), axis=0)

    count = [counts[0, c] for c in range(nclass)]
    for low in range(nclass):
        live = nclass - low

        def body(_, carry, low=low, live=live):
            mixed = []
            for rows in tiles:
                t = widen(jnp.tanh(lanes(y_ref, rows)), deep)
                m = jnp.dot(w1_ref[...], split(t), preferred_element_type=F32)
                mixed.append(m[:sp])
            for rows, m in zip(tiles, mixed):
                y = lanes(y_ref, rows)
                g = tall(lanes(r1_ref, rows)) * y - lanes(st_ref, rows) - m
                w2 = w2_ref[: up(live * sp, 16), :]
                out = jnp.dot(w2, split(widen(g, deep)), preferred_element_type=F32)
                kind = tall(lanes(kind_ref, rows))
                step = out[(live - 1) * sp : live * sp] if low == 0 else jnp.zeros_like(y)
                for j in range(live - 1 if low == 0 else live):
                    step = jnp.where(kind == nclass - 1 - j, out[j * sp : (j + 1) * sp], step)
                y = y - step
                for i, r in enumerate(rows):
                    y_ref[r] = y[:, i * nz : (i + 1) * nz]
            return carry

        begin = 0 if low == 0 else count[low - 1]
        lax.fori_loop(begin, count[low], body, 0)


def shifted(v):
    lane = lax.broadcasted_iota(jnp.int32, v.shape, 1)
    nz = v.shape[1]
    left = jnp.where(lane == 0, 0.0, pltpu.roll(v, 1, 1))
    right = jnp.where(lane == nz - 1, 0.0, pltpu.roll(v, nz - 1, 1))
    return left + right


def lap(v, nbrs):
    total = shifted(v) - 6.0 * v
    for other in nbrs:
        total = total + other
    return total


def start_row(i, target, cls, inverse, y_ref, st_ref, r1_ref, kind_ref, nclass):
    sp, nz = target.shape
    kind = jnp.broadcast_to(cls, (SUB, nz))
    inv = inverse[0]
    for c in range(1, nclass):
        inv = jnp.where(kind == c, inverse[c], inv)
    y_ref[i] = target
    st_ref[i] = target * jnp.concatenate([inv] * (sp // SUB), axis=0)
    r1_ref[i] = inv + 1.0
    kind_ref[i] = kind


def exists(axis):
    me, last = lax.axis_index(axis), lax.axis_size(axis) - 1
    return jnp.where(me % 2 == 0, me > 0, me < last)


def faces_kernel(nx, ny, ns, block, cls, fa, fya, fyb):
    xa, far = near_index("gx", nx), far_index("gx", nx)
    for face, index in ((fyb, far_index), (fya, near_index)):
        y, inner = index("gy", ny), index("gy", ny, 1)
        for x in range(nx):
            put(face, (x,), block[pl.ds(x * ny + y, ns, stride=nx * ny), :], ns)
        put(face, (nx,), block[pl.ds(far * ny + inner, ns, stride=nx * ny), :], ns)
        face[nx, ns : ns + 1, :] = cls[far, pl.ds(y, 1), :]
    for s in range(ns):
        fa[pl.ds(s * ny, ny), :] = block[pl.ds(s * nx * ny + xa * ny, ny), :]


def make_scale(scale, dif, ns):
    sp, nz = scale.shape
    sub = lax.broadcasted_iota(jnp.int32, (SUB, nz), 0)
    for g in range(0, sp, SUB):
        value = jnp.zeros((SUB, nz), F32)
        for s in range(g, min(g + SUB, ns)):
            value = jnp.where(sub == s - g, dif[s], value)
        scale[g : g + SUB, :] = value


def make_weights(w1, w2, square, mixing, inverses, rate, ns, sp, nclass):
    deep = square.shape[0]
    square[...] = jnp.zeros_like(square)
    square[:ns, :ns] = mixing[...]
    value = square[...]
    back = value.astype(BF16).astype(F32)
    w1[:, : 2 * deep] = (back + pltpu.roll(back, deep, 1)).astype(BF16)
    w1[:, 2 * deep :] = (value - back).astype(BF16)[:, :deep]
    highs, lows = [], []
    for c in reversed(range(nclass)):
        square[:ns, :ns] = inverses[c] * rate[c]
        value = square[:sp, :]
        back = value.astype(BF16).astype(F32)
        highs.append(back + pltpu.roll(back, deep, 1))
        lows.append(value - back)
    whole = w2.shape[0]
    w2[:, : 2 * deep] = widen(jnp.concatenate(highs, axis=0), whole).astype(BF16)
    w2[:, 2 * deep :] = widen(jnp.concatenate(lows, axis=0), whole).astype(BF16)[:, :deep]


def prep_kernel(nx, ny, ns, nclass, rate, count, dif, block, mixing, inverses, s_ref, scale, w1, w2, inverse, counts, square):
    make_scale(scale, dif, ns)
    lane = lax.broadcasted_iota(jnp.int32, counts.shape, 1)
    found = jnp.zeros(counts.shape, jnp.int32)
    for c in range(nclass):
        inverse[c] = jnp.full(inverse.shape[1:], 1.0 / rate[c], F32)
        found = jnp.where(lane == c, count[c], found)
    counts[...] = found
    make_weights(w1, w2, square, mixing, inverses, rate, ns, s_ref.shape[2], nclass)
    for x in range(nx):
        for y in range(ny):
            put(s_ref, (x, y), block[pl.ds(x * ny + y, ns, stride=nx * ny), :], ns)


def edge_rows(ya, yb):
    even_y = lax.axis_index("gy") % 2 == 0
    return lambda x, high: jnp.where(even_y == high, ya[x], yb[x])


def send_kernel(nx, ny, ns, block, s_ref, ya, yb, cls, scale, message):
    far, inner = far_index("gx", nx), far_index("gx", nx, 1)
    edge = edge_rows(ya, yb)
    for s in range(ns):
        message[pl.ds(s * ny, ny), :] = block[pl.ds(s * nx * ny + far * ny, ny), :]
    for y in range(ny):
        v = s_ref[far, y]
        low = s_ref[far, y - 1] if y > 0 else edge(far, False)
        high = s_ref[far, y + 1] if y < ny - 1 else edge(far, True)
        part = v + scale[...] * lap(v, [s_ref[inner, y], low, high])
        message[pl.ds(ns * ny + y, ns, stride=ny), :] = part[:ns]
    base = 2 * ns * ny
    message[pl.ds(base, ny), :] = cls[far]
    message[pl.ds(base + ny, ns, stride=2), :] = ya[far][:ns]
    message[pl.ds(base + ny + 1, ns, stride=2), :] = yb[far][:ns]


def near_kernel(nx, ny, ns, nclass, inverse, counts, s_ref, halo, ya, yb, cls, scale, w1, w2,
                f_ref, sec, face, fya, fyb, y_ref, st_ref, r1_ref, kind_ref):
    sp, nz = s_ref.shape[2:]
    edge = edge_rows(ya, yb)
    near, inner, far = near_index("gx", nx), near_index("gx", nx, 1), far_index("gx", nx)
    places = [(near, y) for y in range(ny)] + [(x, y) for x in range(1, nx - 1) for y in range(ny)]
    for i, (x, y) in enumerate(places):
        if i < ny:
            nbrs = [s_ref[inner, y], widen(halo[pl.ds(y, ns, stride=ny), :], sp)]
        else:
            nbrs = [s_ref[x - 1, y], s_ref[x + 1, y]]
        nbrs.append(s_ref[x, y - 1] if y > 0 else edge(x, False))
        nbrs.append(s_ref[x, y + 1] if y < ny - 1 else edge(x, True))
        v = s_ref[x, y]
        force = scale[...] * lap(v, nbrs)
        f_ref[x, y] = force
        start_row(i, v + force, cls[x, y : y + 1, :], inverse, y_ref, st_ref, r1_ref, kind_ref, nclass)
    newton(len(places), y_ref, st_ref, r1_ref, kind_ref, counts, w1, w2, nclass)
    for i, (x, y) in enumerate(places):
        sec[x, y] = y_ref[i]
        if i < ny:
            face[pl.ds(y, ns, stride=ny), :] = y_ref[i][:ns]
    for fy, y in ((fya, near_index("gy", ny)), (fyb, far_index("gy", ny))):
        fy[far] = jnp.zeros((sp, nz), F32)
        fy[near] = sec[near, y]
        for x in range(1, nx - 1):
            fy[x] = sec[x, y]


def far_kernel(nx, ny, ns, nclass, inverse, counts, s_ref, message, ya, yb, cls, scale, w1, w2, f_in, sec_in,
               f_ref, sec, beyond, beside, y_ref, st_ref, r1_ref, kind_ref):
    sp = s_ref.shape[2]
    edge = edge_rows(ya, yb)
    far, inner = far_index("gx", nx), far_index("gx", nx, 1)
    base = 2 * ns * ny

    def begin(i, target, kind):
        start_row(i, target, kind, inverse, y_ref, st_ref, r1_ref, kind_ref, nclass)

    for y in range(ny):
        v = s_ref[far, y]
        nbrs = [
            s_ref[inner, y],
            widen(message[pl.ds(y, ns, stride=ny), :], sp),
            s_ref[far, y - 1] if y > 0 else edge(far, False),
            s_ref[far, y + 1] if y < ny - 1 else edge(far, True),
        ]
        force = scale[...] * lap(v, nbrs)
        f_ref[far, y] = force
        begin(y, v + force, cls[far, y : y + 1, :])
        target = widen(message[pl.ds(ns * ny + y, ns, stride=ny), :], sp) + scale[...] * v
        begin(ny + y, target, message[pl.ds(base + y, 1), :])
    for k, (halo, y) in enumerate(((ya, near_index("gy", ny)), (yb, far_index("gy", ny)))):
        v = halo[far]
        corner = widen(message[pl.ds(base + ny + k, ns, stride=2), :], sp)
        target = v + scale[...] * lap(v, [halo[inner], corner, halo[nx], s_ref[far, y]])
        begin(2 * ny + k, target, halo[nx, ns : ns + 1, :])
    newton(2 * ny + 2, y_ref, st_ref, r1_ref, kind_ref, counts, w1, w2, nclass)
    there = exists("gx")
    for y in range(ny):
        sec[far, y] = y_ref[y]
        beyond[y] = jnp.where(there, y_ref[ny + y], 0.0)
    beside[0] = y_ref[2 * ny]
    beside[1] = jnp.where(exists("gy"), y_ref[2 * ny + 1], 0.0)


def last_kernel(nx, ny, ns, sec, f_ref, xa, beyond, ya, yb, beside, scale, out):
    sp = sec.shape[2]
    even_x = lax.axis_index("gx") % 2 == 0
    even_y = lax.axis_index("gy") % 2 == 0

    def outer(y, high):
        near = widen(xa[pl.ds(y, ns, stride=ny), :], sp)
        return jnp.where(even_x == high, near, beyond[y])

    def edge(x, high):
        value = jnp.where(even_y == high, ya[x], yb[x])
        if 0 < x < nx - 1:
            return value
        side = jnp.where(even_y == high, beside[0], beside[1])
        return jnp.where(even_x == (x == 0), side, value)

    for x in range(nx):
        for y in range(ny):
            v = sec[x, y]
            nbrs = [
                sec[x - 1, y] if x > 0 else outer(y, False),
                sec[x + 1, y] if x < nx - 1 else outer(y, True),
                sec[x, y - 1] if y > 0 else edge(x, False),
                sec[x, y + 1] if y < ny - 1 else edge(x, True),
            ]
            value = v + 0.5 * (scale[...] * lap(v, nbrs) - f_ref[x, y])
            out[pl.ds(x * ny + y, ns, stride=nx * ny), :] = value[:ns]


def local(species, diffusion, class_rate, mixing, inverses, newton_counts, cell_class):
    ns, nx, ny, nz = species.shape
    nclass = class_rate.shape[0]
    sp = up(ns + 1, SUB)
    deep = up(sp, 16)
    block = species.reshape(ns * nx * ny, nz)

    def shape(*dims, dtype=F32):
        return jax.ShapeDtypeStruct(dims, dtype)

    field = shape(nx, ny, sp, nz)
    xface = shape(ns * ny, nz)

    def call(kernel, small, big, outs, scratch=(), mib=6, work=1, alias=()):
        return pl.pallas_call(
            kernel,
            out_shape=tuple(outs),
            in_specs=[SMEM] * len(small) + [VMEM] * len(big),
            out_specs=(VMEM,) * len(outs),
            scratch_shapes=list(scratch),
            input_output_aliases=dict(alias),
            compiler_params=pltpu.CompilerParams(vmem_limit_bytes=mib * 2**20),
            cost_estimate=pl.CostEstimate(flops=work, bytes_accessed=1, transcendentals=0),
        )(*small, *big)

    def scratch(n):
        return [
            pltpu.VMEM((n, sp, nz), F32),
            pltpu.VMEM((n, sp, nz), F32),
            pltpu.VMEM((n, SUB, nz), F32),
            pltpu.VMEM((n, SUB, nz), F32),
        ]

    us = 10**9
    part = functools.partial
    rate, count = class_rate, newton_counts
    classes = cell_class.astype(F32)
    fa, fya, fyb = call(
        part(faces_kernel, nx, ny, ns),
        [],
        [block, classes],
        [xface, shape(nx + 1, sp, nz), shape(nx + 1, sp, nz)],
    )
    hyb = swap(fyb, "gy", 1)
    ha = swap(fa, "gx", 0)
    hya = swap(fya, "gy", 0)
    s_ref, scale, w1, w2, inverse, counts = call(
        part(prep_kernel, nx, ny, ns, nclass),
        [rate, count, diffusion],
        [block, mixing, inverses],
        [
            field,
            shape(sp, nz),
            shape(deep, 3 * deep, dtype=BF16),
            shape(up(nclass * sp, 16), 3 * deep, dtype=BF16),
            shape(nclass, SUB, nz),
            shape(SUB, nz, dtype=jnp.int32),
        ],
        [pltpu.VMEM((deep, 2 * deep), F32)],
        work=us,
    )
    (message,) = call(
        part(send_kernel, nx, ny, ns),
        [],
        [block, s_ref, hya, hyb, classes, scale],
        [shape(2 * ns * ny + ny + 2 * ns, nz)],
        work=us // 2,
    )
    message = swap(message, "gx", 1)
    force, sec, fa, fya, fyb = call(
        part(near_kernel, nx, ny, ns, nclass),
        [],
        [inverse, counts, s_ref, ha, hya, hyb, classes, scale, w1, w2],
        [field, field, xface, shape(nx, sp, nz), shape(nx, sp, nz)],
        scratch((nx - 1) * ny),
        mib=14,
        work=6 * us,
    )
    back_ya = swap(fya, "gy", 0)
    ha = swap(fa, "gx", 0)
    back_yb = swap(fyb, "gy", 1)
    force, sec, beyond, beside = call(
        part(far_kernel, nx, ny, ns, nclass),
        [],
        [inverse, counts, s_ref, message, hya, hyb, classes, scale, w1, w2, force, sec],
        [field, field, shape(ny, sp, nz), shape(2, sp, nz)],
        scratch(2 * ny + 2),
        mib=12,
        work=5 * us,
        alias=((10, 0), (11, 1)),
    )
    (out,) = call(
        part(last_kernel, nx, ny, ns),
        [],
        [sec, force, ha, beyond, back_ya, back_yb, beside, scale],
        [shape(*block.shape)],
        work=2 * us,
    )
    return out.reshape(species.shape)


def solution(mesh):
    in_specs = (P(None, "gx", "gy", None), P(), P(), P(), P(), P(), P("gx", "gy", None))
    out_specs = P(None, "gx", "gy", None)


    return jax.shard_map(local, mesh=mesh, in_specs=in_specs, out_specs=out_specs, check_vma=False)
```

```python
import functools

import jax
import jax.numpy as jnp
from jax import lax
from jax.experimental import pallas as pl
from jax.experimental.pallas import tpu as pltpu
from jax.sharding import PartitionSpec as P


F32 = jnp.float32
BF16 = jnp.bfloat16
SUB = 8
SMEM = pl.BlockSpec(memory_space=pltpu.SMEM)
VMEM = pl.BlockSpec(memory_space=pltpu.VMEM)


def up(value, step):
    return -(-value // step) * step


def swap(block, axis, first):
    count = lax.axis_size(axis)
    pairs = []
    for i in range(first, count - 1, 2):
        pairs += [(i, i + 1), (i + 1, i)]
    return lax.ppermute(block, axis, pairs)


def near_index(axis, size, inner=0):
    return jnp.where(lax.axis_index(axis) % 2 == 0, size - 1 - inner, inner)


def far_index(axis, size, inner=0):
    return jnp.where(lax.axis_index(axis) % 2 == 0, inner, size - 1 - inner)


def split(value):
    high = value.astype(BF16)
    low = (value - high.astype(F32)).astype(BF16)
    return jnp.concatenate([high, low, high], axis=0)


def widen(value, rows):
    short = rows - value.shape[0]
    if short == 0:
        return value
    return jnp.concatenate([value, jnp.zeros((short, value.shape[1]), value.dtype)], axis=0)


def put(ref, index, value, rows):
    whole = ref.shape[-2]
    if whole != rows:
        ref[(*index, slice(whole - SUB, whole), slice(None))] = jnp.zeros((SUB, ref.shape[-1]), F32)
    ref[(*index, slice(0, rows), slice(None))] = value


def newton(n, y_ref, st_ref, r1_ref, kind_ref, counts, w1_ref, w2_ref, nclass):
    sp, nz = y_ref.shape[1:]
    deep = w1_ref.shape[0]
    tiles = [list(range(i, min(i + 2, n))) for i in range(0, n, 2)]

    def lanes(ref, rows):
        return jnp.concatenate([ref[r] for r in rows], axis=1)

    def tall(value):
        return jnp.concatenate([value] * (sp // SUB), axis=0)

    count = [counts[0, c] for c in range(nclass)]
    for low in range(nclass):
        live = nclass - low

        def body(_, carry, low=low, live=live):
            mixed = []
            for rows in tiles:
                t = widen(jnp.tanh(lanes(y_ref, rows)), deep)
                m = jnp.dot(w1_ref[...], split(t), preferred_element_type=F32)
                mixed.append(m[:sp])
            for rows, m in zip(tiles, mixed):
                y = lanes(y_ref, rows)
                g = tall(lanes(r1_ref, rows)) * y - lanes(st_ref, rows) - m
                w2 = w2_ref[: up(live * sp, 16), :]
                out = jnp.dot(w2, split(widen(g, deep)), preferred_element_type=F32)
                kind = tall(lanes(kind_ref, rows))
                step = out[(live - 1) * sp : live * sp] if low == 0 else jnp.zeros_like(y)
                for j in range(live - 1 if low == 0 else live):
                    step = jnp.where(kind == nclass - 1 - j, out[j * sp : (j + 1) * sp], step)
                y = y - step
                for i, r in enumerate(rows):
                    y_ref[r] = y[:, i * nz : (i + 1) * nz]
            return carry

        begin = 0 if low == 0 else count[low - 1]
        lax.fori_loop(begin, count[low], body, 0)


def shifted(v):
    lane = lax.broadcasted_iota(jnp.int32, v.shape, 1)
    nz = v.shape[1]
    left = jnp.where(lane == 0, 0.0, pltpu.roll(v, 1, 1))
    right = jnp.where(lane == nz - 1, 0.0, pltpu.roll(v, nz - 1, 1))
    return left + right


def lap(v, nbrs):
    total = shifted(v) - 6.0 * v
    for other in nbrs:
        total = total + other
    return total


def start_row(i, target, cls, inverse, y_ref, st_ref, r1_ref, kind_ref, nclass):
    sp, nz = target.shape
    kind = jnp.broadcast_to(cls, (SUB, nz))
    inv = inverse[0]
    for c in range(1, nclass):
        inv = jnp.where(kind == c, inverse[c], inv)
    y_ref[i] = target
    st_ref[i] = target * jnp.concatenate([inv] * (sp // SUB), axis=0)
    r1_ref[i] = inv + 1.0
    kind_ref[i] = kind


def exists(axis):
    me, last = lax.axis_index(axis), lax.axis_size(axis) - 1
    return jnp.where(me % 2 == 0, me > 0, me < last)


def faces_kernel(nx, ny, ns, block, cls, fa, fya, fyb):
    xa, far = near_index("gx", nx), far_index("gx", nx)
    for face, index in ((fyb, far_index), (fya, near_index)):
        y, inner = index("gy", ny), index("gy", ny, 1)
        for x in range(nx):
            put(face, (x,), block[pl.ds(x * ny + y, ns, stride=nx * ny), :], ns)
        put(face, (nx,), block[pl.ds(far * ny + inner, ns, stride=nx * ny), :], ns)
        face[nx, ns : ns + 1, :] = cls[far, pl.ds(y, 1), :]
    for s in range(ns):
        fa[pl.ds(s * ny, ny), :] = block[pl.ds(s * nx * ny + xa * ny, ny), :]


def make_scale(scale, dif, ns):
    sp, nz = scale.shape
    sub = lax.broadcasted_iota(jnp.int32, (SUB, nz), 0)
    for g in range(0, sp, SUB):
        value = jnp.zeros((SUB, nz), F32)
        for s in range(g, min(g + SUB, ns)):
            value = jnp.where(sub == s - g, dif[s], value)
        scale[g : g + SUB, :] = value


def make_weights(w1, w2, square, mixing, inverses, rate, ns, sp, nclass):
    deep = square.shape[0]
    square[...] = jnp.zeros_like(square)
    square[:ns, :ns] = mixing[...]
    value = square[...]
    back = value.astype(BF16).astype(F32)
    w1[:, : 2 * deep] = (back + pltpu.roll(back, deep, 1)).astype(BF16)
    w1[:, 2 * deep :] = (value - back).astype(BF16)[:, :deep]
    highs, lows = [], []
    for c in reversed(range(nclass)):
        square[:ns, :ns] = inverses[c] * rate[c]
        value = square[:sp, :]
        back = value.astype(BF16).astype(F32)
        highs.append(back + pltpu.roll(back, deep, 1))
        lows.append(value - back)
    whole = w2.shape[0]
    w2[:, : 2 * deep] = widen(jnp.concatenate(highs, axis=0), whole).astype(BF16)
    w2[:, 2 * deep :] = widen(jnp.concatenate(lows, axis=0), whole).astype(BF16)[:, :deep]


def prep_kernel(nx, ny, ns, nclass, rate, count, dif, block, mixing, inverses, s_ref, scale, w1, w2, inverse, counts, square):
    make_scale(scale, dif, ns)
    lane = lax.broadcasted_iota(jnp.int32, counts.shape, 1)
    found = jnp.zeros(counts.shape, jnp.int32)
    for c in range(nclass):
        inverse[c] = jnp.full(inverse.shape[1:], 1.0 / rate[c], F32)
        found = jnp.where(lane == c, count[c], found)
    counts[...] = found
    make_weights(w1, w2, square, mixing, inverses, rate, ns, s_ref.shape[2], nclass)
    for x in range(nx):
        for y in range(ny):
            put(s_ref, (x, y), block[pl.ds(x * ny + y, ns, stride=nx * ny), :], ns)


def edge_rows(ya, yb):
    even_y = lax.axis_index("gy") % 2 == 0
    return lambda x, high: jnp.where(even_y == high, ya[x], yb[x])


def send_kernel(nx, ny, ns, block, s_ref, ya, yb, cls, scale, message):
    far, inner = far_index("gx", nx), far_index("gx", nx, 1)
    edge = edge_rows(ya, yb)
    for s in range(ns):
        message[pl.ds(s * ny, ny), :] = block[pl.ds(s * nx * ny + far * ny, ny), :]
    for y in range(ny):
        v = s_ref[far, y]
        low = s_ref[far, y - 1] if y > 0 else edge(far, False)
        high = s_ref[far, y + 1] if y < ny - 1 else edge(far, True)
        part = v + scale[...] * lap(v, [s_ref[inner, y], low, high])
        message[pl.ds(ns * ny + y, ns, stride=ny), :] = part[:ns]
    base = 2 * ns * ny
    message[pl.ds(base, ny), :] = cls[far]
    message[pl.ds(base + ny, ns, stride=2), :] = ya[far][:ns]
    message[pl.ds(base + ny + 1, ns, stride=2), :] = yb[far][:ns]


def near_kernel(nx, ny, ns, nclass, inverse, counts, s_ref, halo, ya, yb, cls, scale, w1, w2,
                f_ref, sec, face, fya, fyb, y_ref, st_ref, r1_ref, kind_ref):
    sp, nz = s_ref.shape[2:]
    edge = edge_rows(ya, yb)
    near, inner, far = near_index("gx", nx), near_index("gx", nx, 1), far_index("gx", nx)
    places = [(near, y) for y in range(ny)] + [(x, y) for x in range(1, nx - 1) for y in range(ny)]
    for i, (x, y) in enumerate(places):
        if i < ny:
            nbrs = [s_ref[inner, y], widen(halo[pl.ds(y, ns, stride=ny), :], sp)]
        else:
            nbrs = [s_ref[x - 1, y], s_ref[x + 1, y]]
        nbrs.append(s_ref[x, y - 1] if y > 0 else edge(x, False))
        nbrs.append(s_ref[x, y + 1] if y < ny - 1 else edge(x, True))
        v = s_ref[x, y]
        force = scale[...] * lap(v, nbrs)
        f_ref[x, y] = force
        start_row(i, v + force, cls[x, y : y + 1, :], inverse, y_ref, st_ref, r1_ref, kind_ref, nclass)
    newton(len(places), y_ref, st_ref, r1_ref, kind_ref, counts, w1, w2, nclass)
    for i, (x, y) in enumerate(places):
        sec[x, y] = y_ref[i]
        if i < ny:
            face[pl.ds(y, ns, stride=ny), :] = y_ref[i][:ns]
    for fy, y in ((fya, near_index("gy", ny)), (fyb, far_index("gy", ny))):
        fy[far] = jnp.zeros((sp, nz), F32)
        fy[near] = sec[near, y]
        for x in range(1, nx - 1):
            fy[x] = sec[x, y]


def far_kernel(nx, ny, ns, nclass, inverse, counts, s_ref, message, ya, yb, cls, scale, w1, w2, f_in, sec_in,
               f_ref, sec, beyond, beside, y_ref, st_ref, r1_ref, kind_ref):
    sp = s_ref.shape[2]
    edge = edge_rows(ya, yb)
    far, inner = far_index("gx", nx), far_index("gx", nx, 1)
    base = 2 * ns * ny

    def begin(i, target, kind):
        start_row(i, target, kind, inverse, y_ref, st_ref, r1_ref, kind_ref, nclass)

    for y in range(ny):
        v = s_ref[far, y]
        nbrs = [
            s_ref[inner, y],
            widen(message[pl.ds(y, ns, stride=ny), :], sp),
            s_ref[far, y - 1] if y > 0 else edge(far, False),
            s_ref[far, y + 1] if y < ny - 1 else edge(far, True),
        ]
        force = scale[...] * lap(v, nbrs)
        f_ref[far, y] = force
        begin(y, v + force, cls[far, y : y + 1, :])
        target = widen(message[pl.ds(ns * ny + y, ns, stride=ny), :], sp) + scale[...] * v
        begin(ny + y, target, message[pl.ds(base + y, 1), :])
    for k, (halo, y) in enumerate(((ya, near_index("gy", ny)), (yb, far_index("gy", ny)))):
        v = halo[far]
        corner = widen(message[pl.ds(base + ny + k, ns, stride=2), :], sp)
        target = v + scale[...] * lap(v, [halo[inner], corner, halo[nx], s_ref[far, y]])
        begin(2 * ny + k, target, halo[nx, ns : ns + 1, :])
    newton(2 * ny + 2, y_ref, st_ref, r1_ref, kind_ref, counts, w1, w2, nclass)
    there = exists("gx")
    for y in range(ny):
        sec[far, y] = y_ref[y]
        beyond[y] = jnp.where(there, y_ref[ny + y], 0.0)
    beside[0] = y_ref[2 * ny]
    beside[1] = jnp.where(exists("gy"), y_ref[2 * ny + 1], 0.0)


def last_kernel(nx, ny, ns, sec, f_ref, xa, beyond, ya, yb, beside, scale, out, layers, sems):
    sp = sec.shape[2]
    even_x = lax.axis_index("gx") % 2 == 0
    even_y = lax.axis_index("gy") % 2 == 0

    def outer(y, high):
        near = widen(xa[pl.ds(y, ns, stride=ny), :], sp)
        return jnp.where(even_x == high, near, beyond[y])

    def edge(x, high):
        value = jnp.where(even_y == high, ya[x], yb[x])
        if 0 < x < nx - 1:
            return value
        side = jnp.where(even_y == high, beside[0], beside[1])
        return jnp.where(even_x == (x == 0), side, value)

    copies = []
    for x in range(nx):
        layer = layers.at[x].reshape(ns * ny, layers.shape[-1])
        for y in range(ny):
            v = sec[x, y]
            nbrs = [
                sec[x - 1, y] if x > 0 else outer(y, False),
                sec[x + 1, y] if x < nx - 1 else outer(y, True),
                sec[x, y - 1] if y > 0 else edge(x, False),
                sec[x, y + 1] if y < ny - 1 else edge(x, True),
            ]
            value = v + 0.5 * (scale[...] * lap(v, nbrs) - f_ref[x, y])
            layer[pl.ds(y, ns, stride=ny), :] = value[:ns]
        copies.append(pltpu.make_async_copy(layers.at[x], out.at[:, x], sems.at[x]))
        copies[-1].start()
    for copy in copies:
        copy.wait()


def local(species, diffusion, class_rate, mixing, inverses, newton_counts, cell_class):
    ns, nx, ny, nz = species.shape
    nclass = class_rate.shape[0]
    sp = up(ns + 1, SUB)
    deep = up(sp, 16)
    block = species.reshape(ns * nx * ny, nz)

    def shape(*dims, dtype=F32):
        return jax.ShapeDtypeStruct(dims, dtype)

    field = shape(nx, ny, sp, nz)
    xface = shape(ns * ny, nz)

    def call(kernel, small, big, outs, scratch=(), mib=6, work=1, alias=(), place=VMEM):
        return pl.pallas_call(
            kernel,
            out_shape=tuple(outs),
            in_specs=[SMEM] * len(small) + [VMEM] * len(big),
            out_specs=(place,) * len(outs),
            scratch_shapes=list(scratch),
            input_output_aliases=dict(alias),
            compiler_params=pltpu.CompilerParams(vmem_limit_bytes=mib * 2**20),
            cost_estimate=pl.CostEstimate(flops=work, bytes_accessed=1, transcendentals=0),
        )(*small, *big)

    def scratch(n):
        return [
            pltpu.VMEM((n, sp, nz), F32),
            pltpu.VMEM((n, sp, nz), F32),
            pltpu.VMEM((n, SUB, nz), F32),
            pltpu.VMEM((n, SUB, nz), F32),
        ]

    us = 10**9
    part = functools.partial
    rate, count = class_rate, newton_counts
    classes = cell_class.astype(F32)
    fa, fya, fyb = call(
        part(faces_kernel, nx, ny, ns),
        [],
        [block, classes],
        [xface, shape(nx + 1, sp, nz), shape(nx + 1, sp, nz)],
    )
    hyb = swap(fyb, "gy", 1)
    ha = swap(fa, "gx", 0)
    hya = swap(fya, "gy", 0)
    s_ref, scale, w1, w2, inverse, counts = call(
        part(prep_kernel, nx, ny, ns, nclass),
        [rate, count, diffusion],
        [block, mixing, inverses],
        [
            field,
            shape(sp, nz),
            shape(deep, 3 * deep, dtype=BF16),
            shape(up(nclass * sp, 16), 3 * deep, dtype=BF16),
            shape(nclass, SUB, nz),
            shape(SUB, nz, dtype=jnp.int32),
        ],
        [pltpu.VMEM((deep, 2 * deep), F32)],
        work=us,
    )
    (message,) = call(
        part(send_kernel, nx, ny, ns),
        [],
        [block, s_ref, hya, hyb, classes, scale],
        [shape(2 * ns * ny + ny + 2 * ns, nz)],
        work=us // 2,
    )
    message = swap(message, "gx", 1)
    force, sec, fa, fya, fyb = call(
        part(near_kernel, nx, ny, ns, nclass),
        [],
        [inverse, counts, s_ref, ha, hya, hyb, classes, scale, w1, w2],
        [field, field, xface, shape(nx, sp, nz), shape(nx, sp, nz)],
        scratch((nx - 1) * ny),
        mib=14,
        work=6 * us,
    )
    back_ya = swap(fya, "gy", 0)
    ha = swap(fa, "gx", 0)
    back_yb = swap(fyb, "gy", 1)
    force, sec, beyond, beside = call(
        part(far_kernel, nx, ny, ns, nclass),
        [],
        [inverse, counts, s_ref, message, hya, hyb, classes, scale, w1, w2, force, sec],
        [field, field, shape(ny, sp, nz), shape(2, sp, nz)],
        scratch(2 * ny + 2),
        mib=12,
        work=5 * us,
        alias=((10, 0), (11, 1)),
    )
    (out,) = call(
        part(last_kernel, nx, ny, ns),
        [],
        [sec, force, ha, beyond, back_ya, back_yb, beside, scale],
        [shape(ns, nx, ny, nz)],
        [pltpu.VMEM((nx, ns, ny, nz), F32), pltpu.SemaphoreType.DMA((nx,))],
        work=2 * us,
        place=pl.BlockSpec(memory_space=pl.ANY),
    )
    return out


def solution(mesh):
    in_specs = (P(None, "gx", "gy", None), P(), P(), P(), P(), P(), P("gx", "gy", None))
    out_specs = P(None, "gx", "gy", None)


    return jax.shard_map(local, mesh=mesh, in_specs=in_specs, out_specs=out_specs, check_vma=False)
```

```python
import functools

import jax
import jax.numpy as jnp
from jax import lax
from jax.experimental import pallas as pl
from jax.experimental.pallas import tpu as pltpu
from jax.sharding import PartitionSpec as P


F32 = jnp.float32
BF16 = jnp.bfloat16
SUB = 8
SMEM = pl.BlockSpec(memory_space=pltpu.SMEM)
VMEM = pl.BlockSpec(memory_space=pltpu.VMEM)


def up(value, step):
    return -(-value // step) * step


def swap(block, axis, first):
    count = lax.axis_size(axis)
    pairs = []
    for i in range(first, count - 1, 2):
        pairs += [(i, i + 1), (i + 1, i)]
    return lax.ppermute(block, axis, pairs)


def near_index(axis, size, inner=0):
    return jnp.where(lax.axis_index(axis) % 2 == 0, size - 1 - inner, inner)


def far_index(axis, size, inner=0):
    return jnp.where(lax.axis_index(axis) % 2 == 0, inner, size - 1 - inner)


def split(value):
    high = value.astype(BF16)
    low = (value - high.astype(F32)).astype(BF16)
    return jnp.concatenate([high, low, high], axis=0)


def widen(value, rows):
    short = rows - value.shape[0]
    if short == 0:
        return value
    return jnp.concatenate([value, jnp.zeros((short, value.shape[1]), value.dtype)], axis=0)


def put(ref, index, value, rows):
    whole = ref.shape[-2]
    if whole != rows:
        ref[(*index, slice(whole - SUB, whole), slice(None))] = jnp.zeros((SUB, ref.shape[-1]), F32)
    ref[(*index, slice(0, rows), slice(None))] = value


def newton(n, y_ref, st_ref, r1_ref, kind_ref, counts, w1_ref, w2_ref, nclass):
    sp, nz = y_ref.shape[1:]
    deep = w1_ref.shape[0]
    tiles = [list(range(i, min(i + 2, n))) for i in range(0, n, 2)]

    def lanes(ref, rows):
        return jnp.concatenate([ref[r] for r in rows], axis=1)

    def tall(value):
        return jnp.concatenate([value] * (sp // SUB), axis=0)

    count = [counts[0, c] for c in range(nclass)]
    for low in range(nclass):
        live = nclass - low

        def body(_, carry, low=low, live=live):
            mixed = []
            for rows in tiles:
                t = widen(jnp.tanh(lanes(y_ref, rows)), deep)
                m = jnp.dot(w1_ref[...], split(t), preferred_element_type=F32)
                mixed.append(m[:sp])
            for rows, m in zip(tiles, mixed):
                y = lanes(y_ref, rows)
                g = tall(lanes(r1_ref, rows)) * y - lanes(st_ref, rows) - m
                w2 = w2_ref[: up(live * sp, 16), :]
                out = jnp.dot(w2, split(widen(g, deep)), preferred_element_type=F32)
                kind = tall(lanes(kind_ref, rows))
                step = out[(live - 1) * sp : live * sp] if low == 0 else jnp.zeros_like(y)
                for j in range(live - 1 if low == 0 else live):
                    step = jnp.where(kind == nclass - 1 - j, out[j * sp : (j + 1) * sp], step)
                y = y - step
                for i, r in enumerate(rows):
                    y_ref[r] = y[:, i * nz : (i + 1) * nz]
            return carry

        begin = 0 if low == 0 else count[low - 1]
        lax.fori_loop(begin, count[low], body, 0)


def shifted(v):
    lane = lax.broadcasted_iota(jnp.int32, v.shape, 1)
    nz = v.shape[1]
    left = jnp.where(lane == 0, 0.0, pltpu.roll(v, 1, 1))
    right = jnp.where(lane == nz - 1, 0.0, pltpu.roll(v, nz - 1, 1))
    return left + right


def lap(v, nbrs):
    total = shifted(v) - 6.0 * v
    for other in nbrs:
        total = total + other
    return total


def start_row(i, target, cls, inverse, y_ref, st_ref, r1_ref, kind_ref, nclass):
    sp, nz = target.shape
    kind = jnp.broadcast_to(cls, (SUB, nz))
    inv = inverse[0]
    for c in range(1, nclass):
        inv = jnp.where(kind == c, inverse[c], inv)
    y_ref[i] = target
    st_ref[i] = target * jnp.concatenate([inv] * (sp // SUB), axis=0)
    r1_ref[i] = inv + 1.0
    kind_ref[i] = kind


def exists(axis):
    me, last = lax.axis_index(axis), lax.axis_size(axis) - 1
    return jnp.where(me % 2 == 0, me > 0, me < last)


def faces_kernel(nx, ny, ns, block, cls, fa, fya, fyb):
    xa, far = near_index("gx", nx), far_index("gx", nx)
    for face, index in ((fyb, far_index), (fya, near_index)):
        y, inner = index("gy", ny), index("gy", ny, 1)
        for x in range(nx):
            put(face, (x,), block[pl.ds(x * ny + y, ns, stride=nx * ny), :], ns)
        put(face, (nx,), block[pl.ds(far * ny + inner, ns, stride=nx * ny), :], ns)
        face[nx, ns : ns + 1, :] = cls[far, pl.ds(y, 1), :]
    for s in range(ns):
        fa[pl.ds(s * ny, ny), :] = block[pl.ds(s * nx * ny + xa * ny, ny), :]


def make_scale(scale, dif, ns):
    sp, nz = scale.shape
    sub = lax.broadcasted_iota(jnp.int32, (SUB, nz), 0)
    for g in range(0, sp, SUB):
        value = jnp.zeros((SUB, nz), F32)
        for s in range(g, min(g + SUB, ns)):
            value = jnp.where(sub == s - g, dif[s], value)
        scale[g : g + SUB, :] = value


def make_weights(w1, w2, square, mixing, inverses, ns, sp, nclass):
    deep = square.shape[0]
    square[...] = jnp.zeros_like(square)
    square[:ns, :ns] = mixing[...]
    value = square[...]
    back = value.astype(BF16).astype(F32)
    w1[:, : 2 * deep] = (back + pltpu.roll(back, deep, 1)).astype(BF16)
    w1[:, 2 * deep :] = (value - back).astype(BF16)[:, :deep]
    highs, lows = [], []
    for c in range(nclass):
        square[:ns, :ns] = inverses[c]
        value = square[:sp, :]
        back = value.astype(BF16).astype(F32)
        highs.append(back + pltpu.roll(back, deep, 1))
        lows.append(value - back)
    whole = w2.shape[0]
    w2[:, : 2 * deep] = widen(jnp.concatenate(highs, axis=0), whole).astype(BF16)
    w2[:, 2 * deep :] = widen(jnp.concatenate(lows, axis=0), whole).astype(BF16)[:, :deep]


def scale_kernel(ns, nclass, rate, count, dif, scale, rates, counts):
    make_scale(scale, dif, ns)
    lane = lax.broadcasted_iota(jnp.int32, counts.shape, 1)
    found = jnp.zeros(counts.shape, jnp.int32)
    for c in range(nclass):
        rates[c] = jnp.full(rates.shape[1:], 1.0 / rate[c], F32)
        found = jnp.where(lane == c, count[c], found)
    counts[...] = found


def prep_kernel(nx, ny, ns, nclass, block, mixing, inverses, s_ref, w1, w2, square):
    make_weights(w1, w2, square, mixing, inverses, ns, s_ref.shape[2], nclass)
    for x in range(nx):
        for y in range(ny):
            put(s_ref, (x, y), block[pl.ds(x * ny + y, ns, stride=nx * ny), :], ns)


def edge_rows(ya, yb):
    even_y = lax.axis_index("gy") % 2 == 0
    return lambda x, high: jnp.where(even_y == high, ya[x], yb[x])


def send_kernel(nx, ny, ns, block, ya, yb, cls, scale, message, rows):
    far, inner = far_index("gx", nx), far_index("gx", nx, 1)
    edge = edge_rows(ya, yb)
    for s in range(ns):
        message[pl.ds(s * ny, ny), :] = block[pl.ds(s * nx * ny + far * ny, ny), :]
    for y in range(ny):
        put(rows, (y,), message[pl.ds(y, ns, stride=ny), :], ns)
    for y in range(ny):
        v = rows[y]
        low = rows[y - 1] if y > 0 else edge(far, False)
        high = rows[y + 1] if y < ny - 1 else edge(far, True)
        within = widen(block[pl.ds(inner * ny + y, ns, stride=nx * ny), :], rows.shape[1])
        part = v + scale[...] * lap(v, [within, low, high])
        message[pl.ds(ns * ny + y, ns, stride=ny), :] = part[:ns]
    base = 2 * ns * ny
    message[pl.ds(base, ny), :] = cls[far]
    message[pl.ds(base + ny, ns, stride=2), :] = ya[far][:ns]
    message[pl.ds(base + ny + 1, ns, stride=2), :] = yb[far][:ns]


def near_kernel(nx, ny, ns, nclass, inverse, counts, s_ref, halo, ya, yb, cls, scale, w1, w2,
                f_ref, sec, face, fya, fyb, y_ref, st_ref, r1_ref, kind_ref):
    sp, nz = s_ref.shape[2:]
    edge = edge_rows(ya, yb)
    near, inner, far = near_index("gx", nx), near_index("gx", nx, 1), far_index("gx", nx)
    places = [(near, y) for y in range(ny)] + [(x, y) for x in range(1, nx - 1) for y in range(ny)]
    for i, (x, y) in enumerate(places):
        if i < ny:
            nbrs = [s_ref[inner, y], widen(halo[pl.ds(y, ns, stride=ny), :], sp)]
        else:
            nbrs = [s_ref[x - 1, y], s_ref[x + 1, y]]
        nbrs.append(s_ref[x, y - 1] if y > 0 else edge(x, False))
        nbrs.append(s_ref[x, y + 1] if y < ny - 1 else edge(x, True))
        v = s_ref[x, y]
        force = scale[...] * lap(v, nbrs)
        f_ref[x, y] = force
        start_row(i, v + force, cls[x, y : y + 1, :], inverse, y_ref, st_ref, r1_ref, kind_ref, nclass)
    newton(len(places), y_ref, st_ref, r1_ref, kind_ref, counts, w1, w2, nclass)
    for i, (x, y) in enumerate(places):
        sec[x, y] = y_ref[i]
        if i < ny:
            face[pl.ds(y, ns, stride=ny), :] = y_ref[i][:ns]
    for fy, y in ((fya, near_index("gy", ny)), (fyb, far_index("gy", ny))):
        fy[far] = jnp.zeros((sp, nz), F32)
        fy[near] = sec[near, y]
        for x in range(1, nx - 1):
            fy[x] = sec[x, y]


def far_kernel(nx, ny, ns, nclass, inverse, counts, s_ref, message, ya, yb, cls, scale, w1, w2, f_in, sec_in,
               f_ref, sec, beyond, beside, y_ref, st_ref, r1_ref, kind_ref):
    sp = s_ref.shape[2]
    edge = edge_rows(ya, yb)
    far, inner = far_index("gx", nx), far_index("gx", nx, 1)
    base = 2 * ns * ny

    def begin(i, target, kind):
        start_row(i, target, kind, inverse, y_ref, st_ref, r1_ref, kind_ref, nclass)

    for y in range(ny):
        v = s_ref[far, y]
        nbrs = [
            s_ref[inner, y],
            widen(message[pl.ds(y, ns, stride=ny), :], sp),
            s_ref[far, y - 1] if y > 0 else edge(far, False),
            s_ref[far, y + 1] if y < ny - 1 else edge(far, True),
        ]
        force = scale[...] * lap(v, nbrs)
        f_ref[far, y] = force
        begin(y, v + force, cls[far, y : y + 1, :])
        target = widen(message[pl.ds(ns * ny + y, ns, stride=ny), :], sp) + scale[...] * v
        begin(ny + y, target, message[pl.ds(base + y, 1), :])
    for k, (halo, y) in enumerate(((ya, near_index("gy", ny)), (yb, far_index("gy", ny)))):
        v = halo[far]
        corner = widen(message[pl.ds(base + ny + k, ns, stride=2), :], sp)
        target = v + scale[...] * lap(v, [halo[inner], corner, halo[nx], s_ref[far, y]])
        begin(2 * ny + k, target, halo[nx, ns : ns + 1, :])
    newton(2 * ny + 2, y_ref, st_ref, r1_ref, kind_ref, counts, w1, w2, nclass)
    there = exists("gx")
    for y in range(ny):
        sec[far, y] = y_ref[y]
        beyond[y] = jnp.where(there, y_ref[ny + y], 0.0)
    beside[0] = y_ref[2 * ny]
    beside[1] = jnp.where(exists("gy"), y_ref[2 * ny + 1], 0.0)


def last_kernel(nx, ny, ns, sec, f_ref, xa, beyond, ya, yb, beside, scale, out, layers, sems):
    sp = sec.shape[2]
    even_x = lax.axis_index("gx") % 2 == 0
    even_y = lax.axis_index("gy") % 2 == 0

    def outer(y, high):
        near = widen(xa[pl.ds(y, ns, stride=ny), :], sp)
        return jnp.where(even_x == high, near, beyond[y])

    def edge(x, high):
        value = jnp.where(even_y == high, ya[x], yb[x])
        if 0 < x < nx - 1:
            return value
        side = jnp.where(even_y == high, beside[0], beside[1])
        return jnp.where(even_x == (x == 0), side, value)

    copies = []
    for x in range(nx):
        layer = layers.at[x].reshape(ns * ny, layers.shape[-1])
        for y in range(ny):
            v = sec[x, y]
            nbrs = [
                sec[x - 1, y] if x > 0 else outer(y, False),
                sec[x + 1, y] if x < nx - 1 else outer(y, True),
                sec[x, y - 1] if y > 0 else edge(x, False),
                sec[x, y + 1] if y < ny - 1 else edge(x, True),
            ]
            value = v + 0.5 * (scale[...] * lap(v, nbrs) - f_ref[x, y])
            layer[pl.ds(y, ns, stride=ny), :] = value[:ns]
        copies.append(pltpu.make_async_copy(layers.at[x], out.at[:, x], sems.at[x]))
        copies[-1].start()
    for copy in copies:
        copy.wait()


def local(species, diffusion, class_rate, mixing, inverses, newton_counts, cell_class):
    ns, nx, ny, nz = species.shape
    nclass = class_rate.shape[0]
    sp = up(ns + 1, SUB)
    deep = up(sp, 16)
    block = species.reshape(ns * nx * ny, nz)

    def shape(*dims, dtype=F32):
        return jax.ShapeDtypeStruct(dims, dtype)

    field = shape(nx, ny, sp, nz)
    xface = shape(ns * ny, nz)

    def call(kernel, small, big, outs, scratch=(), mib=6, work=1, alias=(), place=VMEM):
        return pl.pallas_call(
            kernel,
            out_shape=tuple(outs),
            in_specs=[SMEM] * len(small) + [VMEM] * len(big),
            out_specs=(place,) * len(outs),
            scratch_shapes=list(scratch),
            input_output_aliases=dict(alias),
            compiler_params=pltpu.CompilerParams(vmem_limit_bytes=mib * 2**20),
            cost_estimate=pl.CostEstimate(flops=work, bytes_accessed=1, transcendentals=0),
        )(*small, *big)

    def scratch(n):
        return [
            pltpu.VMEM((n, sp, nz), F32),
            pltpu.VMEM((n, sp, nz), F32),
            pltpu.VMEM((n, SUB, nz), F32),
            pltpu.VMEM((n, SUB, nz), F32),
        ]

    us = 10**9
    part = functools.partial
    rate, count = class_rate, newton_counts
    classes = cell_class.astype(F32)
    fa, fya, fyb = call(
        part(faces_kernel, nx, ny, ns),
        [],
        [block, classes],
        [xface, shape(nx + 1, sp, nz), shape(nx + 1, sp, nz)],
    )
    hyb = swap(fyb, "gy", 1)
    ha = swap(fa, "gx", 0)
    hya = swap(fya, "gy", 0)
    scale, inverse, counts = call(
        part(scale_kernel, ns, nclass),
        [rate, count, diffusion],
        [],
        [shape(sp, nz), shape(nclass, SUB, nz), shape(SUB, nz, dtype=jnp.int32)],
        work=us // 2,
    )
    (message,) = call(
        part(send_kernel, nx, ny, ns),
        [],
        [block, hya, hyb, classes, scale],
        [shape(2 * ns * ny + ny + 2 * ns, nz)],
        [pltpu.VMEM((ny, sp, nz), F32)],
        work=us // 2,
    )
    message = swap(message, "gx", 1)
    scaled = (inverses * rate[:, None, None])[::-1]
    s_ref, w1, w2 = call(
        part(prep_kernel, nx, ny, ns, nclass),
        [],
        [block, mixing, scaled],
        [field, shape(deep, 3 * deep, dtype=BF16), shape(up(nclass * sp, 16), 3 * deep, dtype=BF16)],
        [pltpu.VMEM((deep, 2 * deep), F32)],
        work=us,
    )
    force, sec, fa, fya, fyb = call(
        part(near_kernel, nx, ny, ns, nclass),
        [],
        [inverse, counts, s_ref, ha, hya, hyb, classes, scale, w1, w2],
        [field, field, xface, shape(nx, sp, nz), shape(nx, sp, nz)],
        scratch((nx - 1) * ny),
        mib=14,
        work=6 * us,
    )
    back_ya = swap(fya, "gy", 0)
    ha = swap(fa, "gx", 0)
    back_yb = swap(fyb, "gy", 1)
    force, sec, beyond, beside = call(
        part(far_kernel, nx, ny, ns, nclass),
        [],
        [inverse, counts, s_ref, message, hya, hyb, classes, scale, w1, w2, force, sec],
        [field, field, shape(ny, sp, nz), shape(2, sp, nz)],
        scratch(2 * ny + 2),
        mib=12,
        work=5 * us,
        alias=((10, 0), (11, 1)),
    )
    (out,) = call(
        part(last_kernel, nx, ny, ns),
        [],
        [sec, force, ha, beyond, back_ya, back_yb, beside, scale],
        [shape(ns, nx, ny, nz)],
        [pltpu.VMEM((nx, ns, ny, nz), F32), pltpu.SemaphoreType.DMA((nx,))],
        work=2 * us,
        place=pl.BlockSpec(memory_space=pl.ANY),
    )
    return out


def solution(mesh):
    in_specs = (P(None, "gx", "gy", None), P(), P(), P(), P(), P(), P("gx", "gy", None))
    out_specs = P(None, "gx", "gy", None)


    return jax.shard_map(local, mesh=mesh, in_specs=in_specs, out_specs=out_specs, check_vma=False)
```

```python
import functools

import jax
import jax.numpy as jnp
from jax import lax
from jax.experimental import pallas as pl
from jax.experimental.pallas import tpu as pltpu
from jax.sharding import PartitionSpec as P


F32 = jnp.float32
BF16 = jnp.bfloat16
SUB = 8
SMEM = pl.BlockSpec(memory_space=pltpu.SMEM)
VMEM = pl.BlockSpec(memory_space=pltpu.VMEM)


def up(value, step):
    return -(-value // step) * step


def swap(block, axis, first):
    count = lax.axis_size(axis)
    pairs = []
    for i in range(first, count - 1, 2):
        pairs += [(i, i + 1), (i + 1, i)]
    return lax.ppermute(block, axis, pairs)


def near_index(axis, size, inner=0):
    return jnp.where(lax.axis_index(axis) % 2 == 0, size - 1 - inner, inner)


def far_index(axis, size, inner=0):
    return jnp.where(lax.axis_index(axis) % 2 == 0, inner, size - 1 - inner)


def split(value):
    high = value.astype(BF16)
    low = (value - high.astype(F32)).astype(BF16)
    return jnp.concatenate([high, low, high], axis=0)


def widen(value, rows):
    short = rows - value.shape[0]
    if short == 0:
        return value
    return jnp.concatenate([value, jnp.zeros((short, value.shape[1]), value.dtype)], axis=0)


def put(ref, index, value, rows):
    whole = ref.shape[-2]
    if whole != rows:
        ref[(*index, slice(whole - SUB, whole), slice(None))] = jnp.zeros((SUB, ref.shape[-1]), F32)
    ref[(*index, slice(0, rows), slice(None))] = value


def newton(n, y_ref, st_ref, r1_ref, kind_ref, counts, w1_ref, w2_ref, nclass):
    sp, nz = y_ref.shape[1:]
    deep = w1_ref.shape[0]
    tiles = [list(range(i, min(i + 6, n))) for i in range(0, n, 6)]

    def lanes(ref, rows):
        return jnp.concatenate([ref[r] for r in rows], axis=1)

    def tall(value):
        return jnp.concatenate([value] * (sp // SUB), axis=0)

    count = [counts[0, c] for c in range(nclass)]
    for low in range(nclass):
        live = nclass - low

        def body(_, carry, low=low, live=live):
            mixed = []
            for rows in tiles:
                t = widen(jnp.tanh(lanes(y_ref, rows)), deep)
                m = jnp.dot(w1_ref[...], split(t), preferred_element_type=F32)
                mixed.append(m[:sp])
            for rows, m in zip(tiles, mixed):
                y = lanes(y_ref, rows)
                g = tall(lanes(r1_ref, rows)) * y - lanes(st_ref, rows) - m
                w2 = w2_ref[: up(live * sp, 16), :]
                out = jnp.dot(w2, split(widen(g, deep)), preferred_element_type=F32)
                kind = tall(lanes(kind_ref, rows))
                step = out[(live - 1) * sp : live * sp] if low == 0 else jnp.zeros_like(y)
                for j in range(live - 1 if low == 0 else live):
                    step = jnp.where(kind == nclass - 1 - j, out[j * sp : (j + 1) * sp], step)
                y = y - step
                for i, r in enumerate(rows):
                    y_ref[r] = y[:, i * nz : (i + 1) * nz]
            return carry

        begin = 0 if low == 0 else count[low - 1]
        lax.fori_loop(begin, count[low], body, 0)


def shifted(v):
    lane = lax.broadcasted_iota(jnp.int32, v.shape, 1)
    nz = v.shape[1]
    left = jnp.where(lane == 0, 0.0, pltpu.roll(v, 1, 1))
    right = jnp.where(lane == nz - 1, 0.0, pltpu.roll(v, nz - 1, 1))
    return left + right


def lap(v, nbrs):
    total = shifted(v) - 6.0 * v
    for other in nbrs:
        total = total + other
    return total


def start_row(i, target, cls, inverse, y_ref, st_ref, r1_ref, kind_ref, nclass):
    sp, nz = target.shape
    kind = jnp.broadcast_to(cls, (SUB, nz))
    inv = inverse[0]
    for c in range(1, nclass):
        inv = jnp.where(kind == c, inverse[c], inv)
    y_ref[i] = target
    st_ref[i] = target * jnp.concatenate([inv] * (sp // SUB), axis=0)
    r1_ref[i] = inv + 1.0
    kind_ref[i] = kind


def exists(axis):
    me, last = lax.axis_index(axis), lax.axis_size(axis) - 1
    return jnp.where(me % 2 == 0, me > 0, me < last)


def classes_kernel(cell_class, classes):
    classes[...] = cell_class[...].astype(F32)


def faces_kernel(nx, ny, ns, block, cls, fa, fya, fyb):
    xa, far = near_index("gx", nx), far_index("gx", nx)
    for face, index in ((fyb, far_index), (fya, near_index)):
        y, inner = index("gy", ny), index("gy", ny, 1)
        for x in range(nx):
            put(face, (x,), block[pl.ds(x * ny + y, ns, stride=nx * ny), :], ns)
        put(face, (nx,), block[pl.ds(far * ny + inner, ns, stride=nx * ny), :], ns)
        face[nx, ns : ns + 1, :] = cls[far, pl.ds(y, 1), :]
    for s in range(ns):
        fa[pl.ds(s * ny, ny), :] = block[pl.ds(s * nx * ny + xa * ny, ny), :]


def make_scale(scale, dif, ns):
    sp, nz = scale.shape
    sub = lax.broadcasted_iota(jnp.int32, (SUB, nz), 0)
    for g in range(0, sp, SUB):
        value = jnp.zeros((SUB, nz), F32)
        for s in range(g, min(g + SUB, ns)):
            value = jnp.where(sub == s - g, dif[s], value)
        scale[g : g + SUB, :] = value


def make_weights(w1, w2, square, mixing, inverses, ns, sp, nclass):
    deep = square.shape[0]
    square[...] = jnp.zeros_like(square)
    square[:ns, :ns] = mixing[...]
    value = square[...]
    back = value.astype(BF16).astype(F32)
    w1[:, : 2 * deep] = (back + pltpu.roll(back, deep, 1)).astype(BF16)
    w1[:, 2 * deep :] = (value - back).astype(BF16)[:, :deep]
    highs, lows = [], []
    for c in range(nclass):
        square[:ns, :ns] = inverses[c]
        value = square[:sp, :]
        back = value.astype(BF16).astype(F32)
        highs.append(back + pltpu.roll(back, deep, 1))
        lows.append(value - back)
    whole = w2.shape[0]
    w2[:, : 2 * deep] = widen(jnp.concatenate(highs, axis=0), whole).astype(BF16)
    w2[:, 2 * deep :] = widen(jnp.concatenate(lows, axis=0), whole).astype(BF16)[:, :deep]


def scale_kernel(ns, nclass, rate, count, dif, mixing, scale, rates, counts, mixed):
    mixed[...] = mixing[...]
    make_scale(scale, dif, ns)
    lane = lax.broadcasted_iota(jnp.int32, counts.shape, 1)
    found = jnp.zeros(counts.shape, jnp.int32)
    for c in range(nclass):
        rates[c] = jnp.full(rates.shape[1:], 1.0 / rate[c], F32)
        found = jnp.where(lane == c, count[c], found)
    counts[...] = found


def prep_kernel(nx, ny, ns, nclass, block, mixing, inverses, s_ref, w1, w2, square):
    make_weights(w1, w2, square, mixing, inverses, ns, s_ref.shape[2], nclass)
    for x in range(nx):
        for y in range(ny):
            put(s_ref, (x, y), block[pl.ds(x * ny + y, ns, stride=nx * ny), :], ns)


def edge_rows(ya, yb):
    even_y = lax.axis_index("gy") % 2 == 0
    return lambda x, high: jnp.where(even_y == high, ya[x], yb[x])


def send_kernel(nx, ny, ns, block, ya, yb, cls, scale, message, rows):
    far, inner = far_index("gx", nx), far_index("gx", nx, 1)
    edge = edge_rows(ya, yb)
    for s in range(ns):
        message[pl.ds(s * ny, ny), :] = block[pl.ds(s * nx * ny + far * ny, ny), :]
    for y in range(ny):
        put(rows, (y,), message[pl.ds(y, ns, stride=ny), :], ns)
    for y in range(ny):
        v = rows[y]
        low = rows[y - 1] if y > 0 else edge(far, False)
        high = rows[y + 1] if y < ny - 1 else edge(far, True)
        within = widen(block[pl.ds(inner * ny + y, ns, stride=nx * ny), :], rows.shape[1])
        part = v + scale[...] * lap(v, [within, low, high])
        message[pl.ds(ns * ny + y, ns, stride=ny), :] = part[:ns]
    base = 2 * ns * ny
    message[pl.ds(base, ny), :] = cls[far]
    message[pl.ds(base + ny, ns, stride=2), :] = ya[far][:ns]
    message[pl.ds(base + ny + 1, ns, stride=2), :] = yb[far][:ns]


def near_kernel(nx, ny, ns, nclass, inverse, counts, s_ref, halo, ya, yb, cls, scale, w1, w2,
                f_ref, sec, face, fya, fyb, y_ref, st_ref, r1_ref, kind_ref):
    sp, nz = s_ref.shape[2:]
    edge = edge_rows(ya, yb)
    near, inner, far = near_index("gx", nx), near_index("gx", nx, 1), far_index("gx", nx)
    places = [(near, y) for y in range(ny)] + [(x, y) for x in range(1, nx - 1) for y in range(ny)]
    for i, (x, y) in enumerate(places):
        if i < ny:
            nbrs = [s_ref[inner, y], widen(halo[pl.ds(y, ns, stride=ny), :], sp)]
        else:
            nbrs = [s_ref[x - 1, y], s_ref[x + 1, y]]
        nbrs.append(s_ref[x, y - 1] if y > 0 else edge(x, False))
        nbrs.append(s_ref[x, y + 1] if y < ny - 1 else edge(x, True))
        v = s_ref[x, y]
        force = scale[...] * lap(v, nbrs)
        f_ref[x, y] = force
        start_row(i, v + force, cls[x, y : y + 1, :], inverse, y_ref, st_ref, r1_ref, kind_ref, nclass)
    newton(len(places), y_ref, st_ref, r1_ref, kind_ref, counts, w1, w2, nclass)
    for i, (x, y) in enumerate(places):
        sec[x, y] = y_ref[i]
        if i < ny:
            face[pl.ds(y, ns, stride=ny), :] = y_ref[i][:ns]
    for fy, y in ((fya, near_index("gy", ny)), (fyb, far_index("gy", ny))):
        fy[far] = jnp.zeros((sp, nz), F32)
        fy[near] = sec[near, y]
        for x in range(1, nx - 1):
            fy[x] = sec[x, y]


def far_kernel(nx, ny, ns, nclass, inverse, counts, s_ref, message, ya, yb, cls, scale, w1, w2, f_in, sec_in,
               f_ref, sec, beyond, beside, y_ref, st_ref, r1_ref, kind_ref):
    sp = s_ref.shape[2]
    edge = edge_rows(ya, yb)
    far, inner = far_index("gx", nx), far_index("gx", nx, 1)
    base = 2 * ns * ny

    def begin(i, target, kind):
        start_row(i, target, kind, inverse, y_ref, st_ref, r1_ref, kind_ref, nclass)

    for y in range(ny):
        v = s_ref[far, y]
        nbrs = [
            s_ref[inner, y],
            widen(message[pl.ds(y, ns, stride=ny), :], sp),
            s_ref[far, y - 1] if y > 0 else edge(far, False),
            s_ref[far, y + 1] if y < ny - 1 else edge(far, True),
        ]
        force = scale[...] * lap(v, nbrs)
        f_ref[far, y] = force
        begin(y, v + force, cls[far, y : y + 1, :])
        target = widen(message[pl.ds(ns * ny + y, ns, stride=ny), :], sp) + scale[...] * v
        begin(ny + y, target, message[pl.ds(base + y, 1), :])
    for k, (halo, y) in enumerate(((ya, near_index("gy", ny)), (yb, far_index("gy", ny)))):
        v = halo[far]
        corner = widen(message[pl.ds(base + ny + k, ns, stride=2), :], sp)
        target = v + scale[...] * lap(v, [halo[inner], corner, halo[nx], s_ref[far, y]])
        begin(2 * ny + k, target, halo[nx, ns : ns + 1, :])
    newton(2 * ny + 2, y_ref, st_ref, r1_ref, kind_ref, counts, w1, w2, nclass)
    there = exists("gx")
    for y in range(ny):
        sec[far, y] = y_ref[y]
        beyond[y] = jnp.where(there, y_ref[ny + y], 0.0)
    beside[0] = y_ref[2 * ny]
    beside[1] = jnp.where(exists("gy"), y_ref[2 * ny + 1], 0.0)


def last_kernel(nx, ny, ns, sec, f_ref, xa, beyond, ya, yb, beside, scale, out, layers, sems):
    sp = sec.shape[2]
    even_x = lax.axis_index("gx") % 2 == 0
    even_y = lax.axis_index("gy") % 2 == 0

    def outer(y, high):
        near = widen(xa[pl.ds(y, ns, stride=ny), :], sp)
        return jnp.where(even_x == high, near, beyond[y])

    def edge(x, high):
        value = jnp.where(even_y == high, ya[x], yb[x])
        if 0 < x < nx - 1:
            return value
        side = jnp.where(even_y == high, beside[0], beside[1])
        return jnp.where(even_x == (x == 0), side, value)

    copies = []
    for x in range(nx):
        layer = layers.at[x].reshape(ns * ny, layers.shape[-1])
        for y in range(ny):
            v = sec[x, y]
            nbrs = [
                sec[x - 1, y] if x > 0 else outer(y, False),
                sec[x + 1, y] if x < nx - 1 else outer(y, True),
                sec[x, y - 1] if y > 0 else edge(x, False),
                sec[x, y + 1] if y < ny - 1 else edge(x, True),
            ]
            value = v + 0.5 * (scale[...] * lap(v, nbrs) - f_ref[x, y])
            layer[pl.ds(y, ns, stride=ny), :] = value[:ns]
        copies.append(pltpu.make_async_copy(layers.at[x], out.at[:, x], sems.at[x]))
        copies[-1].start()
    for copy in copies:
        copy.wait()


def local(species, diffusion, class_rate, mixing, inverses, newton_counts, cell_class):
    ns, nx, ny, nz = species.shape
    nclass = class_rate.shape[0]
    sp = up(ns + 1, SUB)
    deep = up(sp, 16)
    block = species.reshape(ns * nx * ny, nz)

    def shape(*dims, dtype=F32):
        return jax.ShapeDtypeStruct(dims, dtype)

    field = shape(nx, ny, sp, nz)
    xface = shape(ns * ny, nz)

    def call(kernel, small, big, outs, scratch=(), mib=6, work=1, alias=(), place=VMEM):
        return pl.pallas_call(
            kernel,
            out_shape=tuple(outs),
            in_specs=[SMEM] * len(small) + [VMEM] * len(big),
            out_specs=(place,) * len(outs),
            scratch_shapes=list(scratch),
            input_output_aliases=dict(alias),
            compiler_params=pltpu.CompilerParams(vmem_limit_bytes=mib * 2**20),
            cost_estimate=pl.CostEstimate(flops=work, bytes_accessed=1, transcendentals=0),
        )(*small, *big)

    def scratch(n):
        return [
            pltpu.VMEM((n, sp, nz), F32),
            pltpu.VMEM((n, sp, nz), F32),
            pltpu.VMEM((n, SUB, nz), F32),
            pltpu.VMEM((n, SUB, nz), F32),
        ]

    us = 10**9
    part = functools.partial
    rate, count = class_rate, newton_counts
    (classes,) = call(classes_kernel, [], [cell_class], [shape(nx, ny, nz)], work=8 * us)
    fa, fya, fyb = call(
        part(faces_kernel, nx, ny, ns),
        [],
        [block, classes],
        [xface, shape(nx + 1, sp, nz), shape(nx + 1, sp, nz)],
    )
    hyb = swap(fyb, "gy", 1)
    ha = swap(fa, "gx", 0)
    hya = swap(fya, "gy", 0)
    scale, inverse, counts, mixed = call(
        part(scale_kernel, ns, nclass),
        [rate, count, diffusion],
        [mixing],
        [shape(sp, nz), shape(nclass, SUB, nz), shape(SUB, nz, dtype=jnp.int32), shape(ns, ns)],
        work=us // 2,
    )
    (message,) = call(
        part(send_kernel, nx, ny, ns),
        [],
        [block, hya, hyb, classes, scale],
        [shape(2 * ns * ny + ny + 2 * ns, nz)],
        [pltpu.VMEM((ny, sp, nz), F32)],
        work=us // 2,
    )
    message = swap(message, "gx", 1)
    scaled = (inverses * rate[:, None, None])[::-1]
    s_ref, w1, w2 = call(
        part(prep_kernel, nx, ny, ns, nclass),
        [],
        [block, mixed, scaled],
        [field, shape(deep, 3 * deep, dtype=BF16), shape(up(nclass * sp, 16), 3 * deep, dtype=BF16)],
        [pltpu.VMEM((deep, 2 * deep), F32)],
        work=us,
    )
    force, sec, fa, fya, fyb = call(
        part(near_kernel, nx, ny, ns, nclass),
        [],
        [inverse, counts, s_ref, ha, hya, hyb, classes, scale, w1, w2],
        [field, field, xface, shape(nx, sp, nz), shape(nx, sp, nz)],
        scratch((nx - 1) * ny),
        mib=14,
        work=6 * us,
    )
    back_ya = swap(fya, "gy", 0)
    ha = swap(fa, "gx", 0)
    back_yb = swap(fyb, "gy", 1)
    force, sec, beyond, beside = call(
        part(far_kernel, nx, ny, ns, nclass),
        [],
        [inverse, counts, s_ref, message, hya, hyb, classes, scale, w1, w2, force, sec],
        [field, field, shape(ny, sp, nz), shape(2, sp, nz)],
        scratch(2 * ny + 2),
        mib=12,
        work=5 * us,
        alias=((10, 0), (11, 1)),
    )
    (out,) = call(
        part(last_kernel, nx, ny, ns),
        [],
        [sec, force, ha, beyond, back_ya, back_yb, beside, scale],
        [shape(ns, nx, ny, nz)],
        [pltpu.VMEM((nx, ns, ny, nz), F32), pltpu.SemaphoreType.DMA((nx,))],
        work=2 * us,
        place=pl.BlockSpec(memory_space=pl.ANY),
    )
    return out


def solution(mesh):
    in_specs = (P(None, "gx", "gy", None), P(), P(), P(), P(), P(), P("gx", "gy", None))
    out_specs = P(None, "gx", "gy", None)


    return jax.shard_map(local, mesh=mesh, in_specs=in_specs, out_specs=out_specs, check_vma=False)
```
